512 devices in a mesh: img: 2 (over core), row: 8 (over z_lo, x), col: 32 (over z_hi, y).
Axes of the slice: x: 4, y: 8, z: 8 (z_hi: 4, z_lo: 2; z = z_hi * 2 + z_lo), core: 2. Of those that a mesh axis runs over, the one named last changes fastest.
Arguments:
- images: bfloat16 [8, 128, 512], P('img', 'row', 'col'), may hold values from -4 to 4
- filters: bfloat16 [64, 9, 9], replicated, may hold values from -0.625 to 0.625
- hidden_bias: float32 [64], replicated, may hold values from -3 to -1
- visible_unit_bias: float32 [], replicated, may hold values from -0.5 to 0.5
- unit_noise: bfloat16 [8, 128, 32768], P('img', 'row', 'col'), may hold values from 0.019897461 to 0.9765625
Outputs:
- recon: bfloat16 [8, 128, 512], P('img', 'row', 'col')
- grad_filters: float32 [64, 9, 9], replicated
- grad_hidden: float32 [64], replicated
- grad_visible: float32 [], replicated
The draws below stay inside these ranges and needn't reach their ends.
All inputs are finite; a program needn't handle non-finite values.
Results may differ from the reference program's by a relative error of at most 0.0075.
Values may be sent and summed in bfloat16 or wider, within the bound.
No kernel may reach another device: no remote copies, remote signals or barrier semaphores. Data moves between devices by JAX's collectives and lax.ppermute only.
A program may use at most 64 MiB of HBM per device.

```python
import jax
import jax.numpy as jnp
from jax import lax

K = 64
FILT = 9
B = 8
H = 128
W = 512


def level_of(own_key, extent, pieces, least, high):
    def one(axis_at, parts):
        steps = jax.random.uniform(jax.random.fold_in(jax.random.fold_in(own_key, 6), axis_at), (parts,), jnp.float32, least / len(pieces), high / len(pieces))
        return jnp.repeat(jnp.exp(steps), extent[axis_at] // parts).reshape((-1,) + (1,) * (len(extent) - axis_at - 1))

    loudness = one(*pieces[0])
    for cut in pieces[1:]:
        loudness = loudness * one(*cut)
    return loudness


def gaussian(stream_key, shape, deviation, most, cuts=(), dtype=jnp.bfloat16):
    array = deviation * jax.random.normal(stream_key, shape, jnp.float32)
    if cuts:
        array = array * level_of(stream_key, shape, cuts, -0.22, 0.18)
    return jnp.clip(array, -most, most).astype(dtype)


def setup_inputs(seed: int = 0) -> dict:
    arg_keys = jax.random.split(jax.random.key(seed), 6)
    return {
        "images": gaussian(arg_keys[0], (B, H, W), 1.0, 4.0, ((0, 2), (1, 8), (2, 32))),
        "filters": gaussian(arg_keys[1], (K, FILT, FILT), (FILT * FILT) ** -0.5, 0.625),
        "hidden_bias": jnp.clip(jax.random.uniform(arg_keys[2], (K,), jnp.float32, -3.0, -1.0), -3.0, -1.0),
        "visible_unit_bias": jnp.clip(jax.random.uniform(arg_keys[3], (), jnp.float32, -0.5, 0.5), -0.5, 0.5),
        "unit_noise": jnp.clip(0.019897461 + 0.95666504 * jax.random.uniform(arg_keys[4], (B, H, W * K), jnp.float32) ** level_of(arg_keys[4], (B, H, W * K), ((0, 2), (1, 8), (2, 32)), -0.2, 0.2), 0.019897461, 0.9765625).astype(jnp.bfloat16),
    }


relaxation_coldness = 0.5


def group_peak_odds(binary_hidden_outcome):
    axis_ordering = binary_hidden_outcome.shape
    lifted_power = jnp.exp(binary_hidden_outcome).reshape(axis_ordering[0], axis_ordering[1], axis_ordering[2] // 2, 2, axis_ordering[3] // 2, 2)
    denominator = 1.0 + jnp.sum(lifted_power, axis=(3, 5), keepdims=True)
    return (lifted_power / denominator).reshape(axis_ordering)


def smoothed_draw(binary_hidden_outcome, flat_random_numbers):
    random_jitter_draw = -jnp.log(-jnp.log(flat_random_numbers.astype(jnp.float32)))
    return group_peak_odds((binary_hidden_outcome + random_jitter_draw) / relaxation_coldness).astype(jnp.bfloat16)


def cross_correlate(source, kernels, margin):
    return lax.conv_general_dilated(source, kernels, (1, 1), ((margin, margin), (margin, margin)), dimension_numbers=("NCHW", "OIHW", "NCHW"), preferred_element_type=jnp.float32)


def filter_terms(source, hidden_map, margin):
    return lax.conv_general_dilated(source, hidden_map, (1, 1), ((margin, margin), (margin, margin)), dimension_numbers=("NCHW", "IOHW", "NCHW"), preferred_element_type=jnp.float32)[0]


def reference(images, filters, hidden_bias, visible_unit_bias, unit_noise):
    margin = FILT // 2
    kernels = filters[:, None]
    flipped = filters[None, :, ::-1, ::-1]
    bias_map = hidden_bias[None, :, None, None]

    def one_image(inputs):
        visible, noise_flat = inputs
        flat_random_numbers = noise_flat.reshape(H, W, K).transpose(2, 0, 1)
        source = visible[None, None]
        positive = cross_correlate(source, kernels, margin) + bias_map
        pos_prob = group_peak_odds(positive)
        sample = smoothed_draw(positive, flat_random_numbers[None])
        recon = (cross_correlate(sample, flipped, margin)[0, 0] + visible_unit_bias).astype(jnp.bfloat16)
        model_phase_statistics = cross_correlate(recon[None, None], kernels, margin) + bias_map
        neg_prob = group_peak_odds(model_phase_statistics)
        filter_sum = filter_terms(source, pos_prob.astype(jnp.bfloat16), margin) - filter_terms(recon[None, None], neg_prob.astype(jnp.bfloat16), margin)
        hidden_sum = jnp.sum(pos_prob - neg_prob, axis=(0, 2, 3))
        visible_sum = jnp.sum(visible.astype(jnp.float32) - recon.astype(jnp.float32))
        return recon, filter_sum, hidden_sum, visible_sum

    recon, filter_sums, hidden_sums, visible_sums = lax.map(one_image, (images, unit_noise))
    scale = 1.0 / (B * H * W)
    return recon, jnp.sum(filter_sums, axis=0) * scale, jnp.sum(hidden_sums, axis=0) * scale, jnp.sum(visible_sums) * scale
```

```python
import jax
import jax.numpy as jnp
from jax import lax
from jax.experimental import pallas as pl
from jax.experimental.pallas import tpu as pltpu
from jax.sharding import Mesh
from jax.sharding import PartitionSpec as P

ROW = ("row_0", "row_1")
COL = ("col_0", "col_1")
LANES = 128
INTERPRET = False


def call(kernel, out_shape, scratch, name, smem=()):
    outs = out_shape if isinstance(out_shape, (list, tuple)) else (out_shape,)

    def run(*args):
        specs = [
            pl.BlockSpec(memory_space=pltpu.SMEM if at in smem else pltpu.VMEM)
            for at in range(len(args))
        ]
        return pl.pallas_call(
            kernel,
            out_shape=out_shape,
            in_specs=specs,
            out_specs=tuple(pl.BlockSpec(memory_space=pltpu.VMEM) for _ in outs),
            scratch_shapes=scratch,
            name=name,
            interpret=INTERPRET,
        )(*args)

    return run


def edges(axis, tail, head):
    count = lax.axis_size(axis)
    ends = count - 1
    return (
        lax.ppermute(tail, axis, [(i, (i + 1) % count) for i in range(ends)]),
        lax.ppermute(head, axis, [((i + 1) % count, i) for i in range(ends)]),
    )


def extended(cells, sides, width):
    for axis, dim in sides:
        size = cells.shape[dim]
        before, after = edges(
            axis,
            lax.slice_in_dim(cells, size - width, size, axis=dim),
            lax.slice_in_dim(cells, 0, width, axis=dim),
        )
        cells = jnp.concatenate([before, cells, after], axis=dim)
    return cells


def folded(cells, sides, width):
    for axis, dim in sides:
        size = cells.shape[dim]
        before, after = edges(
            axis,
            lax.slice_in_dim(cells, size - width, size, axis=dim),
            lax.slice_in_dim(cells, 0, width, axis=dim),
        )
        middle = list(cells.shape)
        middle[dim] = size - 2 * width
        cells = cells + jnp.concatenate([before, jnp.zeros(middle, cells.dtype), after], axis=dim)
    return cells


def summed(x, axes):
    count = lax.axis_size(axes)
    parts = lax.all_to_all(
        jnp.broadcast_to(x[None], (count,) + x.shape), axes, 0, 0, tiled=True
    )
    return jnp.sum(parts, axis=0)


def block_sum(x):
    x = x + pltpu.roll(x, x.shape[1] // 2, 1)
    rows = x.shape[0]
    even = lax.broadcasted_iota(jnp.int32, x.shape, 0) % 2 == 0
    return x + jnp.where(even, pltpu.roll(x, rows - 1, 0), pltpu.roll(x, 1, 0))


def body(images, filters, hidden_bias, visible_unit_bias, unit_noise):
    n_img, tile_rows, tile_cols = images.shape
    channels, side, _ = filters.shape
    margin = side // 2
    high, wide = tile_rows + 2 * margin, tile_cols + 2 * margin
    rows = n_img * tile_rows
    units = tile_cols * channels
    taps = side * wide
    chunks = units // LANES
    f32, bf16 = jnp.float32, jnp.bfloat16

    def patches(wide_ref, out_ref):
        for n in range(n_img):
            out_ref[n * tile_rows : (n + 1) * tile_rows, :] = jnp.concatenate(
                [wide_ref[n, r : r + tile_rows, :] for r in range(side)], axis=1
            )

    def prep_kernel(pair_ref, noise_ref, w_ref, t_ref, wide_ref):
        wide_ref[...] = jnp.zeros_like(wide_ref)
        for r in range(side):
            block = pair_ref[r]
            for v in range(chunks):
                wide_ref[pl.ds(r * wide + 2 * v, side + 1), pl.ds(v * LANES, LANES)] = block
        w_ref[...] = wide_ref[...].astype(bf16)
        t_ref[...] = 1.0 / jnp.log(noise_ref[...].astype(f32))

    def up_kernel(vis_ref, w_ref, t_ref, bias_ref, part_ref, prob_ref, a_ref, hid_ref, img_ref, col_ref, samp_ref):
        img_ref[...] = vis_ref[...].astype(f32)
        patches(img_ref, col_ref)
        a_ref[...] = col_ref[...].astype(bf16)
        a = a_ref[...]
        for v in range(chunks):
            at = slice(v * LANES, (v + 1) * LANES)
            act = jnp.dot(a, w_ref[:, at], preferred_element_type=f32) + bias_ref[...]
            lift = jnp.exp(act)
            prob = lift / (1.0 + block_sum(lift))
            prob_ref[:, at] = prob.astype(bf16)
            hid_ref[:, at] = jnp.sum(prob, axis=0, keepdims=True)
            cold = lift * t_ref[:, at]
            cold = cold * cold
            samp_ref[:, at] = (cold / (1.0 + block_sum(cold))).astype(bf16)
        down = lax.dot_general(
            samp_ref[...], w_ref[...], (((1,), (1,)), ((), ())), preferred_element_type=f32
        )
        part_ref[...] = jnp.zeros_like(part_ref)
        for r in range(side):
            piece = down[:, r * wide : (r + 1) * wide]
            for n in range(n_img):
                part_ref[n, r : r + tile_rows, :] += piece[n * tile_rows : (n + 1) * tile_rows]

    def down_kernel(
        edge_ref, vb_ref, tot_ref, vis_ref, w_ref, bias_ref, prob_ref, a_ref, hid_ref,
        recon_ref, pack_ref, img_ref, col_ref, a2_ref, p2_ref, g_ref, cmb_ref,
    ):
        p = lax.broadcasted_iota(jnp.int32, (n_img, high, wide), 1)
        q = lax.broadcasted_iota(jnp.int32, (n_img, high, wide), 2)
        inside = (p >= edge_ref[0]) & (p < edge_ref[1]) & (q >= edge_ref[2]) & (q < edge_ref[3])
        recon = (tot_ref[...] + vb_ref[0]).astype(bf16).astype(f32)
        recon = jnp.where(inside, recon, 0.0)
        img_ref[...] = recon
        mine = img_ref[:, margin : margin + tile_rows, margin : margin + tile_cols]
        recon_ref[...] = mine.astype(bf16)
        seen = jnp.sum(jnp.sum(vis_ref[...].astype(f32) - mine, axis=0), keepdims=True)
        patches(img_ref, col_ref)
        a2_ref[:rows, :] = a_ref[...]
        a2_ref[rows:, :] = -col_ref[...].astype(bf16)
        p2_ref[:rows, :] = prob_ref[...]
        a = col_ref[...].astype(bf16)
        hidden = jnp.zeros((1, LANES), f32)
        for v in range(chunks):
            at = slice(v * LANES, (v + 1) * LANES)
            act = jnp.dot(a, w_ref[:, at], preferred_element_type=f32) + bias_ref[...]
            lift = jnp.exp(act)
            prob = lift / (1.0 + block_sum(lift))
            p2_ref[rows:, at] = prob.astype(bf16)
            hidden = hidden + (hid_ref[:, at] - jnp.sum(prob, axis=0, keepdims=True))
        g_ref[...] = lax.dot_general(
            a2_ref[...], p2_ref[...], (((0,), (0,)), ((), ())), preferred_element_type=f32
        )
        for r in range(side):
            acc = g_ref[pl.ds(r * wide, side + 1), pl.ds(0, LANES)]
            for v in range(1, chunks):
                acc = acc + g_ref[pl.ds(r * wide + 2 * v, side + 1), pl.ds(v * LANES, LANES)]
            half = pltpu.roll(acc, channels, 1)
            cmb_ref[r * side : (r + 1) * side, :] = acc[:side] + half[1 : side + 1]
        count = side * side
        first = (count + 1) // 2
        lane = lax.broadcasted_iota(jnp.int32, (first, LANES), 1)
        lower = cmb_ref[:first, :]
        upper = pltpu.roll(cmb_ref[count - first : count, :], channels, 1)
        pack_ref[...] = jnp.zeros_like(pack_ref)
        pack_ref[:first, :] = jnp.where(lane < channels, lower, upper)
        hidden = hidden + pltpu.roll(hidden, channels, 1)
        lane = lax.broadcasted_iota(jnp.int32, (1, LANES), 1)
        pack_ref[first : first + 1, :] = jnp.where(lane < channels, hidden, seen)

    taps_first = filters.astype(f32).transpose(1, 2, 0)
    pairs = jnp.concatenate(
        [jnp.pad(taps_first, ((0, 0), (0, 1), (0, 0))), jnp.pad(taps_first, ((0, 0), (1, 0), (0, 0)))],
        axis=2,
    )
    bias = jnp.concatenate([hidden_bias, hidden_bias])[None]
    shape = jax.ShapeDtypeStruct
    w, t = call(
        prep_kernel,
        (shape((taps, units), bf16), shape((rows, units), f32)),
        [pltpu.VMEM((taps, units), f32)],
        "prep",
    )(pairs, unit_noise.reshape(rows, units))

    visible_wide = extended(images, ((ROW, 1), (COL, 2)), margin)
    part, prob, a, hid = call(
        up_kernel,
        (
            shape((n_img, high, wide), f32),
            shape((rows, units), bf16),
            shape((rows, taps), bf16),
            shape((1, units), f32),
        ),
        [
            pltpu.VMEM((n_img, high, wide), f32),
            pltpu.VMEM((rows, taps), f32),
            pltpu.VMEM((rows, units), bf16),
        ],
        "up",
    )(visible_wide, w, t, bias)

    total = folded(part, ((ROW, 1), (COL, 2)), 2 * margin)

    def limits(axis, size, extent):
        at, last = lax.axis_index(axis), lax.axis_size(axis) - 1
        return [jnp.where(at == 0, margin, 0), jnp.where(at == last, size + margin, extent)]

    bounds = jnp.stack(limits(ROW, tile_rows, high) + limits(COL, tile_cols, wide)).astype(jnp.int32)
    n_pack = -(-((side * side + 1) // 2 + 1) // 8) * 8
    recon, pack = call(
        down_kernel,
        (shape(images.shape, bf16), shape((n_pack, LANES), f32)),
        [
            pltpu.VMEM((n_img, high, wide), f32),
            pltpu.VMEM((rows, taps), f32),
            pltpu.VMEM((2 * rows, taps), bf16),
            pltpu.VMEM((2 * rows, units), bf16),
            pltpu.VMEM((taps, units), f32),
            pltpu.VMEM((side * side, LANES), f32),
        ],
        "down",
        smem=(0, 1),
    )(bounds, visible_unit_bias[None], total, images, w, bias, prob, a, hid)

    for axes in (("img", "row_1"), "col_1", ("col_0", "row_0")):
        pack = summed(pack, axes)
    scale = 1.0 / float(
        rows * tile_cols * lax.axis_size("img") * lax.axis_size(ROW) * lax.axis_size(COL)
    )
    count = side * side
    first = (count + 1) // 2
    pack = pack * scale
    grad = jnp.concatenate([pack[:first, :channels], pack[2 * first - count : first, channels:]], axis=0)
    grad = grad.T.reshape(channels, side, side)
    return (recon, grad, pack[first, :channels], pack[first, channels])


def solution(mesh):
    split = Mesh(
        mesh.devices.reshape(mesh.shape["img"], 2, 4, 4, 8),
        ("img", "row_0", "row_1", "col_0", "col_1"),
    )
    placed = (P("img", ROW, COL), P(), P(), P(), P("img", ROW, COL))
    return jax.shard_map(
        body,
        mesh=split,
        in_specs=placed,
        out_specs=(P("img", ROW, COL), P(), P(), P()),
        check_vma=False,
    )
```

```python
import jax
import jax.numpy as jnp
from jax import lax
from jax.experimental import pallas as pl
from jax.experimental.pallas import tpu as pltpu
from jax.sharding import Mesh
from jax.sharding import PartitionSpec as P

ROW = ("row_0", "row_1")
COL = ("col_0", "col_1")
LANES = 128
INTERPRET = False
GRANT = 8 << 20


def call(kernel, out_shape, scratch, name, smem=()):
    outs = out_shape if isinstance(out_shape, (list, tuple)) else (out_shape,)

    def run(*args):
        specs = [
            pl.BlockSpec(memory_space=pltpu.SMEM if at in smem else pltpu.VMEM)
            for at in range(len(args))
        ]
        return pl.pallas_call(
            kernel,
            out_shape=out_shape,
            in_specs=specs,
            out_specs=tuple(pl.BlockSpec(memory_space=pltpu.VMEM) for _ in outs),
            scratch_shapes=scratch,
            compiler_params=pltpu.CompilerParams(vmem_limit_bytes=GRANT),
            name=name,
            interpret=INTERPRET,
        )(*args)

    return run


def edges(axis, tail, head):
    count = lax.axis_size(axis)
    ends = count - 1
    return (
        lax.ppermute(tail, axis, [(i, (i + 1) % count) for i in range(ends)]),
        lax.ppermute(head, axis, [((i + 1) % count, i) for i in range(ends)]),
    )


def block_sum(x):
    x = x + pltpu.roll(x, x.shape[1] // 2, 1)
    rows = x.shape[0]
    even = lax.broadcasted_iota(jnp.int32, x.shape, 0) % 2 == 0
    return x + jnp.where(even, pltpu.roll(x, rows - 1, 0), pltpu.roll(x, 1, 0))


def body(images, filters, hidden_bias, visible_unit_bias, unit_noise):
    n_img, tile_rows, tile_cols = images.shape
    channels, side, _ = filters.shape
    margin = side // 2
    reach = 2 * margin
    far = 3 * margin
    high, wide = tile_rows + 2 * margin, tile_cols + 2 * margin
    tall = tile_rows + 2 * reach
    rows = n_img * tile_rows
    units = tile_cols * channels
    taps = side * wide
    chunks = units // LANES
    lower = (side + 1) // 2 * side
    used = lower + 1
    n_pack = -(-(used + 1) // 16) * 16
    f32, bf16 = jnp.float32, jnp.bfloat16
    shape = jax.ShapeDtypeStruct

    def patches(wide_ref, out_ref, count):
        for n in range(n_img):
            out_ref[n * count : (n + 1) * count, :] = jnp.concatenate(
                [wide_ref[n, r : r + count, :] for r in range(side)], axis=1
            )

    def band_kernel(pair_ref, w_ref, wide_ref):
        wide_ref[...] = jnp.zeros_like(wide_ref)
        for r in range(side):
            block = pair_ref[r]
            for v in range(chunks):
                wide_ref[pl.ds(r * wide + 2 * v, side + 1), pl.ds(v * LANES, LANES)] = block
        w_ref[...] = wide_ref[...].astype(bf16)

    def draw_kernel(noise_ref, before_ref, after_ref, t_ref):
        def inverse(u):
            u = u.astype(f32)
            return jnp.where(u > 0.0, 1.0 / jnp.log(u), 0.0)

        for n in range(n_img):
            t_ref[n, :reach, :] = inverse(before_ref[n, :, :units])
            t_ref[n, reach : reach + tile_rows, :] = inverse(noise_ref[n])
            t_ref[n, reach + tile_rows :, :] = inverse(after_ref[n, :, :units])

    def up_kernel(
        vis_ref, w_ref, t_ref, bias_ref,
        part_ref, head_ref, tail_ref, prob_ref, a_ref, hid_ref, img_ref, col_ref, samp_ref, down_ref,
    ):
        img_ref[...] = vis_ref[...].astype(f32)
        patches(img_ref, col_ref, tall)
        a = col_ref[...].astype(bf16)
        for n in range(n_img):
            at = n * tall + reach
            a_ref[n * tile_rows : (n + 1) * tile_rows, :] = col_ref[at : at + tile_rows, :].astype(bf16)
        for v in range(chunks):
            at = slice(v * LANES, (v + 1) * LANES)
            act = jnp.dot(a, w_ref[:, at], preferred_element_type=f32) + bias_ref[...]
            lift = jnp.exp(act)
            hidden = jnp.zeros((1, LANES), f32)
            for n in range(n_img):
                mine = lift[n * tall + reach : n * tall + reach + tile_rows]
                prob = mine / (1.0 + block_sum(mine))
                prob_ref[n * tile_rows : (n + 1) * tile_rows, at] = prob.astype(bf16)
                hidden = hidden + jnp.sum(prob, axis=0, keepdims=True)
            hid_ref[:, at] = hidden
            t = t_ref[:, :, at].reshape(n_img * tall, LANES)
            cold = jnp.where(t == 0.0, 0.0, lift * t)
            cold = cold * cold
            samp_ref[:, at] = (cold / (1.0 + block_sum(cold))).astype(bf16)
        down_ref[...] = lax.dot_general(
            samp_ref[...], w_ref[...], (((1,), (1,)), ((), ())), preferred_element_type=f32
        )
        for n in range(n_img):
            total = jnp.zeros((high, wide), f32)
            for r in range(side):
                at = n * tall + reach - r
                total = total + down_ref[at : at + high, r * wide : (r + 1) * wide]
            part_ref[n] = total
            head_ref[n] = total[:, :reach]
            tail_ref[n] = total[:, wide - reach :]

    def down_kernel(
        edge_ref, vb_ref, part_ref, before_ref, after_ref, vis_ref, w_ref, bias_ref, prob_ref, a_ref, hid_ref,
        recon_ref, pack_ref, img_ref, col_ref, a2_ref, p2_ref, g_ref, cmb_ref, sum_ref,
    ):
        p = lax.broadcasted_iota(jnp.int32, (high, wide), 0)
        q = lax.broadcasted_iota(jnp.int32, (high, wide), 1)
        inside = (p >= edge_ref[0]) & (p < edge_ref[1]) & (q >= edge_ref[2]) & (q < edge_ref[3])
        gap = jnp.zeros((high, wide - 2 * reach), f32)
        seen = jnp.zeros((tile_rows, tile_cols), f32)
        for n in range(n_img):
            total = part_ref[n] + jnp.concatenate([before_ref[n], gap, after_ref[n]], axis=1)
            recon = (total + vb_ref[0]).astype(bf16).astype(f32)
            img_ref[n] = jnp.where(inside, recon, 0.0)
            mine = img_ref[n, margin : margin + tile_rows, margin : margin + tile_cols]
            recon_ref[n] = mine.astype(bf16)
            seen = seen + (vis_ref[n].astype(f32) - mine)
        seen = jnp.sum(seen, keepdims=True)
        patches(img_ref, col_ref, tile_rows)
        a = col_ref[...].astype(bf16)
        a2_ref[:rows, :] = a_ref[...]
        a2_ref[rows:, :] = -a
        p2_ref[:rows, :] = prob_ref[...]
        hidden = jnp.zeros((1, LANES), f32)
        for v in range(chunks):
            at = slice(v * LANES, (v + 1) * LANES)
            act = jnp.dot(a, w_ref[:, at], preferred_element_type=f32) + bias_ref[...]
            lift = jnp.exp(act)
            prob = lift / (1.0 + block_sum(lift))
            p2_ref[rows:, at] = prob.astype(bf16)
            hidden = hidden + (hid_ref[:, at] - jnp.sum(prob, axis=0, keepdims=True))
        g_ref[...] = lax.dot_general(
            a2_ref[...], p2_ref[...], (((0,), (0,)), ((), ())), preferred_element_type=f32
        )
        for r in range(side):
            acc = g_ref[pl.ds(r * wide, side + 1), pl.ds(0, LANES)]
            for v in range(1, chunks):
                acc = acc + g_ref[pl.ds(r * wide + 2 * v, side + 1), pl.ds(v * LANES, LANES)]
            half = pltpu.roll(acc, channels, 1)
            first = acc[:side] + half[1 : side + 1]
            second = half[:side] + acc[1 : side + 1]
            lane = lax.broadcasted_iota(jnp.int32, (side, LANES), 1)
            cmb_ref[r * side : (r + 1) * side, :] = jnp.where(lane < channels, first, second)
        upper = side * side - lower
        lane = lax.broadcasted_iota(jnp.int32, (lower, LANES), 1)
        sum_ref[...] = jnp.zeros_like(sum_ref)
        sum_ref[:lower, :] = jnp.where(lane < channels, cmb_ref[:lower, :], 0.0)
        lane = lax.broadcasted_iota(jnp.int32, (upper, LANES), 1)
        sum_ref[:upper, :] += jnp.where(lane < channels, 0.0, cmb_ref[lower:, :])
        hidden = hidden + pltpu.roll(hidden, channels, 1)
        lane = lax.broadcasted_iota(jnp.int32, (1, LANES), 1)
        last = jnp.where(lane < channels, hidden, seen)
        sum_ref[lower:used, :] = last
        sum_ref[used : used + 1, :] = last - last.astype(bf16).astype(f32)
        packed = sum_ref[...].astype(bf16)
        for at in range(pack_ref.shape[0]):
            pack_ref[at] = packed

    def spread_kernel(parts_ref, pack_ref, sum_ref):
        sum_ref[...] = jnp.sum(parts_ref[...].astype(f32), axis=0)
        last = sum_ref[lower:used, :] + sum_ref[used : used + 1, :]
        sum_ref[lower:used, :] = last
        sum_ref[used : used + 1, :] = last - last.astype(bf16).astype(f32)
        packed = sum_ref[...].astype(bf16)
        for at in range(pack_ref.shape[0]):
            pack_ref[at] = packed

    def finish_kernel(parts_ref, grad_ref, hid_ref, seen_ref, sum_ref):
        sum_ref[...] = jnp.sum(parts_ref[...].astype(f32), axis=0) * scale
        last = sum_ref[lower:used, :] + sum_ref[used : used + 1, :]
        hid_ref[...] = last[:, :channels]
        seen_ref[...] = last[:, channels : channels + 1]
        for r in range(side):
            half, at = (0, r * side) if r * side < lower else (channels, r * side - lower)
            grad_ref[r] = sum_ref[at : at + side, half : half + channels]

    taps_first = filters.astype(f32).transpose(1, 2, 0)
    pairs = jnp.concatenate(
        [jnp.pad(taps_first, ((0, 0), (0, 1), (0, 0))), jnp.pad(taps_first, ((0, 0), (1, 0), (0, 0)))],
        axis=2,
    )
    bias = jnp.concatenate([hidden_bias, hidden_bias])[None]
    (w,) = call(
        band_kernel, (shape((taps, units), bf16),), [pltpu.VMEM((taps, units), f32)], "band"
    )(pairs)

    def joined(noise, pixels):
        more = jnp.pad(pixels[:, reach:], ((0, 0), (0, 2 * reach - far), (0, 0)))
        return jnp.concatenate([noise, pixels[:, :reach], more], axis=2)

    def pixels_of(payload):
        return jnp.concatenate(
            [payload[:, :, units : units + tile_cols], payload[:, : far - reach, units + tile_cols :]], axis=1
        )

    before, after = edges(
        ROW,
        joined(unit_noise[:, tile_rows - reach :], images[:, tile_rows - far :]),
        joined(unit_noise[:, :reach], images[:, :far]),
    )
    column = jnp.concatenate([pixels_of(before), images, pixels_of(after)], axis=1)
    left, right = edges(COL, column[:, :, tile_cols - margin :], column[:, :, :margin])
    (t,) = call(draw_kernel, (shape((n_img, tall, units), f32),), [], "draw")(unit_noise, before, after)
    visible_wide = jnp.concatenate([left, column, right], axis=2)
    part, head, tail, prob, a, hid = call(
        up_kernel,
        (
            shape((n_img, high, wide), f32),
            shape((n_img, high, reach), f32),
            shape((n_img, high, reach), f32),
            shape((rows, units), bf16),
            shape((rows, taps), bf16),
            shape((1, units), f32),
        ),
        [
            pltpu.VMEM(visible_wide.shape, f32),
            pltpu.VMEM((n_img * tall, taps), f32),
            pltpu.VMEM((n_img * tall, units), bf16),
            pltpu.VMEM((n_img * tall, taps), f32),
        ],
        "up",
    )(visible_wide, w, t, bias)

    left, right = edges(COL, tail, head)

    def limits(axis, size, extent):
        at, last = lax.axis_index(axis), lax.axis_size(axis) - 1
        return [jnp.where(at == 0, margin, 0), jnp.where(at == last, size + margin, extent)]

    bounds = jnp.stack(limits(ROW, tile_rows, high) + limits(COL, tile_cols, wide)).astype(jnp.int32)
    groups = (("img", "row_1"), "col_1", ("col_0", "row_0"))
    copies = [lax.axis_size(axes) for axes in groups]
    recon, pack = call(
        down_kernel,
        (shape(images.shape, bf16), shape((copies[0], n_pack, LANES), bf16)),
        [
            pltpu.VMEM((n_img, high, wide), f32),
            pltpu.VMEM((rows, taps), f32),
            pltpu.VMEM((2 * rows, taps), bf16),
            pltpu.VMEM((2 * rows, units), bf16),
            pltpu.VMEM((taps, units), f32),
            pltpu.VMEM((side * side, LANES), f32),
            pltpu.VMEM((n_pack, LANES), f32),
        ],
        "down",
        smem=(0, 1),
    )(bounds, visible_unit_bias[None], part, left, right, images, w, bias, prob, a, hid)

    scale = 1.0 / float(
        rows * tile_cols * lax.axis_size("img") * lax.axis_size(ROW) * lax.axis_size(COL)
    )
    for axes, following in zip(groups, copies[1:] + [None]):
        parts = lax.all_to_all(pack, axes, 0, 0, tiled=True)
        scratch = [pltpu.VMEM((n_pack, LANES), f32)]
        if following:
            (pack,) = call(spread_kernel, (shape((following, n_pack, LANES), bf16),), scratch, "spread")(parts)
    grad, hidden, seen = call(
        finish_kernel,
        (shape((side, side, channels), f32), shape((1, channels), f32), shape((1, 1), f32)),
        scratch,
        "finish",
    )(parts)
    return (recon, grad.transpose(2, 0, 1), hidden[0], seen[0, 0])


def solution(mesh):
    split = Mesh(
        mesh.devices.reshape(mesh.shape["img"], 2, 4, 4, 8),
        ("img", "row_0", "row_1", "col_0", "col_1"),
    )
    placed = (P("img", ROW, COL), P(), P(), P(), P("img", ROW, COL))
    return jax.shard_map(
        body,
        mesh=split,
        in_specs=placed,
        out_specs=(P("img", ROW, COL), P(), P(), P()),
        check_vma=False,
    )
```

```python
import jax
import jax.numpy as jnp
from jax import lax
from jax.experimental import pallas as pl
from jax.experimental.pallas import tpu as pltpu
from jax.sharding import Mesh
from jax.sharding import PartitionSpec as P

ROW = ("row_0", "row_1")
COL = ("col_0", "col_1")
LANES = 128
GROUPS = (("img", "col_1"), ("row_1", "col_0", "row_0"))
INTERPRET = False
GRANT = 8 << 20


def call(kernel, out_shape, scratch, name, smem=()):
    outs = out_shape if isinstance(out_shape, (list, tuple)) else (out_shape,)

    def run(*args):
        specs = [
            pl.BlockSpec(memory_space=pltpu.SMEM if at in smem else pltpu.VMEM)
            for at in range(len(args))
        ]
        return pl.pallas_call(
            kernel,
            out_shape=out_shape,
            in_specs=specs,
            out_specs=tuple(pl.BlockSpec(memory_space=pltpu.VMEM) for _ in outs),
            scratch_shapes=scratch,
            compiler_params=pltpu.CompilerParams(vmem_limit_bytes=GRANT),
            name=name,
            interpret=INTERPRET,
        )(*args)

    return run


def edges(axis, tail, head):
    count = lax.axis_size(axis)
    ends = count - 1
    return (
        lax.ppermute(tail, axis, [(i, (i + 1) % count) for i in range(ends)]),
        lax.ppermute(head, axis, [((i + 1) % count, i) for i in range(ends)]),
    )


def block_sum(x):
    x = x + pltpu.roll(x, x.shape[1] // 2, 1)
    rows = x.shape[0]
    even = lax.broadcasted_iota(jnp.int32, x.shape, 0) % 2 == 0
    return x + jnp.where(even, pltpu.roll(x, rows - 1, 0), pltpu.roll(x, 1, 0))


def body(images, filters, hidden_bias, visible_unit_bias, unit_noise):
    n_img, tile_rows, tile_cols = images.shape
    channels, side, _ = filters.shape
    margin = side // 2
    reach = 2 * margin
    far = 3 * margin
    high = tile_rows + 2 * margin
    tall, taller = tile_rows + 2 * reach, tile_rows + 2 * far
    broad = tile_cols + margin
    wide = broad + 2 * margin
    rows = n_img * tile_rows
    own, units, extra = tile_cols * channels, broad * channels, margin * channels
    taps = side * wide
    chunks, edge = units // LANES, extra // LANES
    count = side * side
    quarter = -(-count // 4)
    part_rows = -(-(quarter + 2) // 8) * 8
    f32, bf16 = jnp.float32, jnp.bfloat16
    shape = jax.ShapeDtypeStruct
    scale = 1.0 / float(
        rows * tile_cols * lax.axis_size("img") * lax.axis_size(ROW) * lax.axis_size(COL)
    )

    def patches(wide_ref, out_ref, size):
        for n in range(n_img):
            out_ref[n * size : (n + 1) * size, :] = jnp.concatenate(
                [wide_ref[n, r : r + size, :] for r in range(side)], axis=1
            )

    def pack_kernel(vis_ref, noise_ref, down_ref, up_ref):
        def beside(first, last, size):
            more = jnp.concatenate([last, jnp.zeros((size - last.shape[0], tile_cols), f32)], axis=0)
            return jnp.concatenate([first, more], axis=1).astype(bf16)

        for n in range(n_img):
            pixels = vis_ref[n].astype(f32)
            down_ref[n, :, :own] = noise_ref[n, tile_rows - reach :, :]
            lowest = pixels[tile_rows - far :]
            down_ref[n, :, own:] = beside(lowest[:reach], lowest[reach:], reach)
            up_ref[n, :, :own] = noise_ref[n, :reach, :]
            up_ref[n, :, own:] = beside(pixels[:reach], pixels[reach:far], reach)

    def mid_kernel(vis_ref, noise_ref, before_ref, after_ref, column_ref, send_ref, col_ref):
        for n in range(n_img):
            for at, payload in ((0, before_ref), (far + tile_rows, after_ref)):
                pixels = payload[n, :, own:].astype(f32)
                col_ref[at : at + reach, :] = pixels[:, :tile_cols]
                col_ref[at + reach : at + far, :] = pixels[: far - reach, tile_cols:]
            col_ref[far : far + tile_rows, :] = vis_ref[n].astype(f32)
            column_ref[n] = col_ref[...].astype(bf16)
            send_ref[n, :reach, :extra] = before_ref[n, :, :extra]
            send_ref[n, reach : reach + tile_rows, :extra] = noise_ref[n, :, :extra]
            send_ref[n, reach + tile_rows :, :extra] = after_ref[n, :, :extra]
            over = taller - tall
            low = jnp.concatenate(
                [col_ref[tall:, :reach], jnp.zeros((tall - over, reach), f32)], axis=0
            )
            send_ref[n, :, extra:] = jnp.concatenate([col_ref[:tall, :reach], low], axis=1).astype(bf16)

    def band_kernel(pair_ref, w_ref, wide_ref):
        wide_ref[...] = jnp.zeros_like(wide_ref)
        for r in range(side):
            block = pair_ref[r]
            for v in range(chunks):
                wide_ref[pl.ds(r * wide + 2 * v, side + 1), pl.ds(v * LANES, LANES)] = block
        w_ref[...] = wide_ref[...].astype(bf16)

    def inverse(u):
        u = u.astype(f32)
        return jnp.where(u > 0.0, 1.0 / jnp.log(u), 0.0)

    def draw_kernel(noise_ref, before_ref, after_ref, t_ref):
        for n in range(n_img):
            t_ref[n, :reach, :] = inverse(before_ref[n, :, :own])
            t_ref[n, reach : reach + tile_rows, :] = inverse(noise_ref[n])
            t_ref[n, reach + tile_rows :, :] = inverse(after_ref[n, :, :own])

    def up_kernel(
        flag_ref, column_ref, next_ref, w_ref, t_ref, bias_ref,
        part_ref, send_ref, prob_ref, a_ref, hid_ref, img_ref, col_ref, samp_ref, down_ref,
    ):
        starts, goes_on = flag_ref[0:1, :], flag_ref[3:4, :]
        for n in range(n_img):
            pixels = next_ref[n, :, extra:].astype(f32)
            beyond = jnp.concatenate([pixels[:, :reach], pixels[: taller - tall, reach:]], axis=0)
            img_ref[n] = jnp.concatenate(
                [jnp.zeros((taller, margin), f32), column_ref[n].astype(f32), beyond], axis=1
            )
        patches(img_ref, col_ref, tall)
        a = col_ref[...].astype(bf16)
        for n in range(n_img):
            at = n * tall + reach
            a_ref[n * tile_rows : (n + 1) * tile_rows, :] = col_ref[at : at + tile_rows, :].astype(bf16)
        for v in range(chunks):
            at = slice(v * LANES, (v + 1) * LANES)
            act = jnp.dot(a, w_ref[:, at], preferred_element_type=f32) + bias_ref[...]
            lift = jnp.exp(act)
            hidden = jnp.zeros((1, LANES), f32)
            for n in range(n_img):
                mine = lift[n * tall + reach : n * tall + reach + tile_rows]
                prob = mine / (1.0 + block_sum(mine))
                if v < edge:
                    prob = jnp.where(starts > 0.0, prob, 0.0)
                if v >= chunks - edge:
                    prob = jnp.where(goes_on > 0.0, prob, 0.0)
                prob_ref[n * tile_rows : (n + 1) * tile_rows, at] = prob.astype(bf16)
                hidden = hidden + jnp.sum(prob, axis=0, keepdims=True)
            hid_ref[:, at] = hidden
            if v >= chunks - edge:
                far_at = slice(v * LANES - own, (v + 1) * LANES - own)
                t = inverse(next_ref[:, :, far_at]).reshape(n_img * tall, LANES)
            else:
                t = t_ref[:, :, at].reshape(n_img * tall, LANES)
            if v < edge:
                t = t * starts
            cold = jnp.where(t == 0.0, 0.0, lift * t)
            cold = cold * cold
            samp_ref[:, at] = (cold / (1.0 + block_sum(cold))).astype(bf16)
        down_ref[...] = lax.dot_general(
            samp_ref[...], w_ref[...], (((1,), (1,)), ((), ())), preferred_element_type=f32
        )
        for n in range(n_img):
            total = jnp.zeros((high, wide), f32)
            for r in range(side):
                at = n * tall + reach - r
                total = total + down_ref[at : at + high, r * wide : (r + 1) * wide]
            part_ref[n] = total[:, margin : margin + tile_cols]
            send_ref[n] = total[:, wide - 2 * reach :]

    def down_kernel(
        flag_ref, part_ref, before_ref, vis_ref, w_ref, bias_ref, prob_ref, a_ref, hid_ref,
        recon_ref, pack_ref, img_ref, col_ref, a2_ref, p2_ref, g_ref, cmb_ref, sum_ref,
    ):
        follows, ends = flag_ref[1:2, :], flag_ref[2:3, :]
        p = lax.broadcasted_iota(jnp.int32, (high, wide), 0)
        q = lax.broadcasted_iota(jnp.int32, (high, wide), 1)
        inside = (
            ((p >= margin) | (flag_ref[4:5, :wide] == 0.0))
            & ((p < margin + tile_rows) | (flag_ref[5:6, :wide] == 0.0))
            & ((q >= reach) | (follows[:, :wide] > 0.0))
            & (q < reach + tile_cols)
        )
        seen = jnp.zeros((tile_rows, tile_cols), f32)
        for n in range(n_img):
            total = jnp.concatenate(
                [before_ref[n], jnp.zeros((high, wide - 2 * reach), f32)], axis=1
            ) + jnp.concatenate(
                [jnp.zeros((high, reach), f32), part_ref[n], jnp.zeros((high, wide - reach - tile_cols), f32)],
                axis=1,
            )
            recon = (total + flag_ref[6:7, :wide]).astype(bf16).astype(f32)
            img_ref[n] = jnp.where(inside, recon, 0.0)
            mine = img_ref[n, margin : margin + tile_rows, reach : reach + tile_cols]
            recon_ref[n] = mine.astype(bf16)
            seen = seen + (vis_ref[n].astype(f32) - mine)
        seen = jnp.sum(seen, keepdims=True)
        patches(img_ref, col_ref, tile_rows)
        a = col_ref[...].astype(bf16)
        a2_ref[:rows, :] = a_ref[...]
        a2_ref[rows:, :] = -a
        p2_ref[:rows, :] = prob_ref[...]
        hidden = jnp.zeros((1, LANES), f32)
        for v in range(chunks):
            at = slice(v * LANES, (v + 1) * LANES)
            act = jnp.dot(a, w_ref[:, at], preferred_element_type=f32) + bias_ref[...]
            lift = jnp.exp(act)
            prob = lift / (1.0 + block_sum(lift))
            if v < edge:
                prob = jnp.where(follows > 0.0, prob, 0.0)
            if v >= chunks - edge:
                prob = jnp.where(ends > 0.0, prob, 0.0)
            p2_ref[rows:, at] = prob.astype(bf16)
            hidden = hidden + (hid_ref[:, at] - jnp.sum(prob, axis=0, keepdims=True))
        g_ref[...] = lax.dot_general(
            a2_ref[...], p2_ref[...], (((0,), (0,)), ((), ())), preferred_element_type=f32
        )
        lane = lax.broadcasted_iota(jnp.int32, (side, LANES), 1)
        cmb_ref[...] = jnp.zeros_like(cmb_ref)
        for r in range(side):
            acc = g_ref[pl.ds(r * wide, side + 1), pl.ds(0, LANES)]
            for v in range(1, chunks):
                acc = acc + g_ref[pl.ds(r * wide + 2 * v, side + 1), pl.ds(v * LANES, LANES)]
            half = pltpu.roll(acc, channels, 1)
            cmb_ref[r * side : (r + 1) * side, :] = jnp.where(
                lane < channels, acc[:side] + half[1 : side + 1], half[:side] + acc[1 : side + 1]
            )
        hidden = hidden + pltpu.roll(hidden, channels, 1)
        lane = lax.broadcasted_iota(jnp.int32, (quarter, LANES), 1)
        copies = pack_ref.shape[0] // 2
        for half, last in ((0, hidden), (1, jnp.broadcast_to(seen, (1, LANES)))):
            at = 2 * half * quarter
            sum_ref[...] = jnp.zeros_like(sum_ref)
            sum_ref[:quarter, :] = jnp.where(
                lane < channels, cmb_ref[at : at + quarter, :], cmb_ref[at + quarter : at + 2 * quarter, :]
            )
            packed = split(sum_ref, last)
            for to in range(copies):
                pack_ref[half * copies + to] = packed

    def split(sum_ref, last):
        sum_ref[quarter : quarter + 1, :] = last
        sum_ref[quarter + 1 : quarter + 2, :] = last - last.astype(bf16).astype(f32)
        return sum_ref[...].astype(bf16)

    def added(parts_ref, sum_ref):
        sum_ref[...] = jnp.sum(parts_ref[...].astype(f32), axis=0)
        return sum_ref[quarter : quarter + 1, :] + sum_ref[quarter + 1 : quarter + 2, :]

    def spread_kernel(parts_ref, pack_ref, sum_ref):
        packed = split(sum_ref, added(parts_ref, sum_ref))
        for to in range(pack_ref.shape[0]):
            pack_ref[to] = packed

    def share_kernel(parts_ref, pack_ref, sum_ref):
        last = added(parts_ref, sum_ref)
        sum_ref[quarter : quarter + 1, :] = last
        for to in range(pack_ref.shape[0]):
            pack_ref[to] = sum_ref[...] * scale

    def finish_kernel(halves_ref, recon_in_ref, recon_ref, grad_ref, hid_ref, seen_ref, flat_ref):
        recon_ref[...] = recon_in_ref[...]
        for half in range(2):
            for side_of in range(2):
                at = (2 * half + side_of) * quarter
                flat_ref[at : at + quarter, :] = halves_ref[
                    half, :quarter, side_of * channels : (side_of + 1) * channels
                ]
        for r in range(side):
            grad_ref[r] = flat_ref[r * side : (r + 1) * side, :]
        hid_ref[...] = halves_ref[0, quarter : quarter + 1, :channels]
        seen_ref[...] = halves_ref[1, quarter : quarter + 1, :1]

    taps_first = filters.astype(f32).transpose(1, 2, 0)
    pairs = jnp.concatenate(
        [jnp.pad(taps_first, ((0, 0), (0, 1), (0, 0))), jnp.pad(taps_first, ((0, 0), (1, 0), (0, 0)))],
        axis=2,
    )
    bias = jnp.concatenate([hidden_bias, hidden_bias])[None]
    col_at, row_at = lax.axis_index(COL), lax.axis_index(ROW)
    first, last = col_at == 0, col_at == lax.axis_size(COL) - 1
    top, bottom = row_at == 0, row_at == lax.axis_size(ROW) - 1
    line = lax.broadcasted_iota(jnp.int32, (8, LANES), 0)
    flags = jnp.zeros((8, LANES), f32)
    for at, value in enumerate(
        (first, ~first, last, ~last, top, bottom, visible_unit_bias)
    ):
        flags = jnp.where(line == at, jnp.asarray(value, f32), flags)

    payload = shape((n_img, reach, own + 2 * tile_cols), bf16)
    downward, upward = call(pack_kernel, (payload, payload), [], "pack")(images, unit_noise)
    before, after = edges(ROW, downward, upward)
    (w,) = call(
        band_kernel, (shape((taps, units), bf16),), [pltpu.VMEM((taps, units), f32)], "band"
    )(pairs)
    column, leftward = call(
        mid_kernel,
        (shape((n_img, taller, tile_cols), bf16), shape((n_img, tall, extra + 2 * reach), bf16)),
        [pltpu.VMEM((taller, tile_cols), f32)],
        "mid",
    )(images, unit_noise, before, after)

    steps = lax.axis_size(COL) - 1
    beyond = lax.ppermute(leftward, COL, [(i + 1, i) for i in range(steps)])
    (t,) = call(draw_kernel, (shape((n_img, tall, own), f32),), [], "draw")(unit_noise, before, after)
    part, rightward, prob, a, hid = call(
        up_kernel,
        (
            shape((n_img, high, tile_cols), f32),
            shape((n_img, high, 2 * reach), f32),
            shape((rows, units), bf16),
            shape((rows, taps), bf16),
            shape((1, units), f32),
        ),
        [
            pltpu.VMEM((n_img, taller, wide), f32),
            pltpu.VMEM((n_img * tall, taps), f32),
            pltpu.VMEM((n_img * tall, units), bf16),
            pltpu.VMEM((n_img * tall, taps), f32),
        ],
        "up",
    )(flags, column, beyond, w, t, bias)

    shares = lax.ppermute(rightward, COL, [(i, i + 1) for i in range(steps)])
    sizes = [lax.axis_size(axes) for axes in GROUPS]
    recon, pack = call(
        down_kernel,
        (shape(images.shape, bf16), shape((sizes[0], part_rows, LANES), bf16)),
        [
            pltpu.VMEM((n_img, high, wide), f32),
            pltpu.VMEM((rows, taps), f32),
            pltpu.VMEM((2 * rows, taps), bf16),
            pltpu.VMEM((2 * rows, units), bf16),
            pltpu.VMEM((taps, units), f32),
            pltpu.VMEM((4 * quarter, LANES), f32),
            pltpu.VMEM((part_rows, LANES), f32),
        ],
        "down",
    )(flags, part, shares, images, w, bias, prob, a, hid)

    scratch = [pltpu.VMEM((part_rows, LANES), f32)]
    for axes, following in zip(GROUPS, sizes[1:] + [None]):
        parts = lax.all_to_all(pack, axes, 0, 0, tiled=True)
        if following:
            (pack,) = call(
                spread_kernel, (shape((following, part_rows, LANES), bf16),), scratch, "spread"
            )(parts)
    (pack,) = call(share_kernel, (shape((2, part_rows, LANES), f32),), scratch, "share")(parts)
    halves = lax.all_to_all(pack, "img", 0, 0, tiled=True)
    recon, grad, hidden, seen = call(
        finish_kernel,
        (
            shape(images.shape, bf16),
            shape((side, side, channels), f32),
            shape((1, channels), f32),
            shape((1, 1), f32),
        ),
        [pltpu.VMEM((4 * quarter, channels), f32)],
        "finish",
    )(halves, recon)
    return (recon, grad.transpose(2, 0, 1), hidden[0], seen[0, 0])


def solution(mesh):
    split = Mesh(
        mesh.devices.reshape(mesh.shape["img"], 2, 4, 4, 8),
        ("img", "row_0", "row_1", "col_0", "col_1"),
    )
    placed = (P("img", ROW, COL), P(), P(), P(), P("img", ROW, COL))
    return jax.shard_map(
        body,
        mesh=split,
        in_specs=placed,
        out_specs=(P("img", ROW, COL), P(), P(), P()),
        check_vma=False,
    )
```

```python
import jax
import jax.numpy as jnp
from jax import lax
from jax.experimental import pallas as pl
from jax.experimental.pallas import tpu as pltpu
from jax.sharding import Mesh
from jax.sharding import PartitionSpec as P

ROW = ("row_0", "row_1")
COL = ("col_0", "col_1")
LANES = 128
GROUPS = (("img", "row_1"), ("col_1",), ("row_0", "col_0"))
INTERPRET = False
GRANT = 8 << 20


def call(kernel, out_shape, scratch, name, left=()):
    outs = out_shape if isinstance(out_shape, (list, tuple)) else (out_shape,)

    def run(*args):
        specs = [
            pl.BlockSpec(memory_space=pltpu.HBM if at in left else pltpu.VMEM)
            for at in range(len(args))
        ]
        return pl.pallas_call(
            kernel,
            out_shape=out_shape,
            in_specs=specs,
            out_specs=tuple(pl.BlockSpec(memory_space=pltpu.VMEM) for _ in outs),
            scratch_shapes=scratch,
            compiler_params=pltpu.CompilerParams(vmem_limit_bytes=GRANT),
            name=name,
            interpret=INTERPRET,
        )(*args)

    return run


def in_hbm(x):
    return x if INTERPRET else pltpu.with_memory_space_constraint(x, pltpu.HBM)


def edges(axis, tail, head):
    count = lax.axis_size(axis)
    ends = count - 1
    return (
        lax.ppermute(tail, axis, [(i, (i + 1) % count) for i in range(ends)]),
        lax.ppermute(head, axis, [((i + 1) % count, i) for i in range(ends)]),
    )


def block_sum(x):
    x = x + pltpu.roll(x, x.shape[1] // 2, 1)
    rows = x.shape[0]
    even = lax.broadcasted_iota(jnp.int32, x.shape, 0) % 2 == 0
    return x + jnp.where(even, pltpu.roll(x, rows - 1, 0), pltpu.roll(x, 1, 0))


def body(images, filters, hidden_bias, visible_unit_bias, unit_noise):
    n_img, tile_rows, tile_cols = images.shape
    channels, side, _ = filters.shape
    margin = side // 2
    reach = 2 * margin
    far = 3 * margin
    high = tile_rows + 2 * margin
    tall, taller = tile_rows + 2 * reach, tile_rows + 2 * far
    broad = tile_cols + margin
    wide = broad + 2 * margin
    rows = n_img * tile_rows
    own, units, extra = tile_cols * channels, broad * channels, margin * channels
    taps = side * wide
    chunks, edge = units // LANES, extra // LANES
    count = side * side
    quarter = -(-count // 4)
    half_rows = -(-(quarter + 2) // 8) * 8
    part_rows = 2 * half_rows
    f32, bf16 = jnp.float32, jnp.bfloat16
    shape = jax.ShapeDtypeStruct
    scale = 1.0 / float(
        rows * tile_cols * lax.axis_size("img") * lax.axis_size(ROW) * lax.axis_size(COL)
    )

    def patches(wide_ref, out_ref, size):
        for n in range(n_img):
            out_ref[n * size : (n + 1) * size, :] = jnp.concatenate(
                [wide_ref[n, r : r + size, :] for r in range(side)], axis=1
            )

    def pack_kernel(vis_hbm, noise_hbm, down_ref, up_ref, vis_ref, sems):
        moves = [
            pltpu.make_async_copy(vis_hbm, vis_ref, sems.at[0]),
            pltpu.make_async_copy(
                noise_hbm.at[:, pl.ds(tile_rows - reach, reach), :], down_ref.at[:, :, pl.ds(0, own)], sems.at[1]
            ),
            pltpu.make_async_copy(
                noise_hbm.at[:, pl.ds(0, reach), :], up_ref.at[:, :, pl.ds(0, own)], sems.at[2]
            ),
        ]
        for move in moves:
            move.start()
        moves[0].wait()

        def beside(first, last, size):
            more = jnp.concatenate([last, jnp.zeros((size - last.shape[0], tile_cols), f32)], axis=0)
            return jnp.concatenate([first, more], axis=1).astype(bf16)

        for n in range(n_img):
            pixels = vis_ref[n].astype(f32)
            lowest = pixels[tile_rows - far :]
            down_ref[n, :, own:] = beside(lowest[:reach], lowest[reach:], reach)
            up_ref[n, :, own:] = beside(pixels[:reach], pixels[reach:far], reach)
        for move in moves[1:]:
            move.wait()

    def mid_kernel(vis_ref, noise_ref, before_ref, after_ref, column_ref, send_ref, col_ref):
        for n in range(n_img):
            for at, payload in ((0, before_ref), (far + tile_rows, after_ref)):
                pixels = payload[n, :, own:].astype(f32)
                col_ref[at : at + reach, :] = pixels[:, :tile_cols]
                col_ref[at + reach : at + far, :] = pixels[: far - reach, tile_cols:]
            col_ref[far : far + tile_rows, :] = vis_ref[n].astype(f32)
            column_ref[n] = col_ref[...].astype(bf16)
            send_ref[n, :reach, :] = before_ref[n, :, :extra]
            send_ref[n, reach : reach + tile_rows, :] = noise_ref[n, :, :extra]
            send_ref[n, reach + tile_rows : tall, :] = after_ref[n, :, :extra]
            blocks = [col_ref[at : at + reach, :reach] for at in range(0, taller, reach)]
            blocks.append(jnp.zeros((reach, extra - taller), f32))
            send_ref[n, tall:, :] = jnp.concatenate(blocks, axis=1).astype(bf16)

    def band_kernel(pair_ref, w_ref, wide_ref):
        wide_ref[...] = jnp.zeros_like(wide_ref)
        for r in range(side):
            block = pair_ref[r]
            for v in range(chunks):
                wide_ref[pl.ds(r * wide + 2 * v, side + 1), pl.ds(v * LANES, LANES)] = block
        w_ref[...] = wide_ref[...].astype(bf16)

    def inverse(u):
        u = u.astype(f32)
        return jnp.where(u > 0.0, 1.0 / jnp.log(u), 0.0)

    def draw_kernel(noise_ref, before_ref, after_ref, t_ref):
        for n in range(n_img):
            t_ref[n, :reach, :] = inverse(before_ref[n, :, :own])
            t_ref[n, reach : reach + tile_rows, :] = inverse(noise_ref[n])
            t_ref[n, reach + tile_rows :, :] = inverse(after_ref[n, :, :own])

    def up_kernel(
        flag_ref, column_ref, next_ref, w_ref, t_ref, bias_ref,
        part_ref, send_ref, prob_ref, a_ref, hid_ref, img_ref, col_ref, samp_ref, down_ref,
    ):
        starts, goes_on = flag_ref[0:1, :], flag_ref[3:4, :]
        for n in range(n_img):
            pixels = next_ref[n, tall:, :].astype(f32)
            beyond = jnp.concatenate(
                [pixels[:, at : at + reach] for at in range(0, taller, reach)], axis=0
            )
            img_ref[n] = jnp.concatenate(
                [jnp.zeros((taller, margin), f32), column_ref[n].astype(f32), beyond], axis=1
            )
        patches(img_ref, col_ref, tall)
        a = col_ref[...].astype(bf16)
        for n in range(n_img):
            at = n * tall + reach
            a_ref[n * tile_rows : (n + 1) * tile_rows, :] = col_ref[at : at + tile_rows, :].astype(bf16)
        for v in range(chunks):
            at = slice(v * LANES, (v + 1) * LANES)
            act = jnp.dot(a, w_ref[:, at], preferred_element_type=f32) + bias_ref[...]
            lift = jnp.exp(act)
            hidden = jnp.zeros((1, LANES), f32)
            for n in range(n_img):
                mine = lift[n * tall + reach : n * tall + reach + tile_rows]
                prob = mine / (1.0 + block_sum(mine))
                if v < edge:
                    prob = jnp.where(starts > 0.0, prob, 0.0)
                if v >= chunks - edge:
                    prob = jnp.where(goes_on > 0.0, prob, 0.0)
                prob_ref[n * tile_rows : (n + 1) * tile_rows, at] = prob.astype(bf16)
                hidden = hidden + jnp.sum(prob, axis=0, keepdims=True)
            hid_ref[:, at] = hidden
            if v >= chunks - edge:
                far_at = slice(v * LANES - own, (v + 1) * LANES - own)
                t = inverse(next_ref[:, :tall, far_at]).reshape(n_img * tall, LANES)
            else:
                t = t_ref[:, :, at].reshape(n_img * tall, LANES)
            if v < edge:
                t = t * starts
            cold = jnp.where(t == 0.0, 0.0, lift * t)
            cold = cold * cold
            samp_ref[:, at] = (cold / (1.0 + block_sum(cold))).astype(bf16)
        down_ref[...] = lax.dot_general(
            samp_ref[...], w_ref[...], (((1,), (1,)), ((), ())), preferred_element_type=f32
        )
        shares = []
        for n in range(n_img):
            total = jnp.zeros((high, wide), f32)
            for r in range(side):
                at = n * tall + reach - r
                total = total + down_ref[at : at + high, r * wide : (r + 1) * wide]
            part_ref[n] = total[:, margin : margin + tile_cols]
            shares.append(total[:, wide - 2 * reach :])
        send_ref[...] = jnp.concatenate(shares, axis=1)

    def down_kernel(
        flag_ref, part_ref, before_ref, vis_ref, w_ref, bias_ref, prob_ref, a_ref, hid_ref,
        recon_ref, pack_ref, img_ref, col_ref, a2_ref, p2_ref, g_ref, cmb_ref, sum_ref,
    ):
        follows, ends = flag_ref[1:2, :], flag_ref[2:3, :]
        p = lax.broadcasted_iota(jnp.int32, (high, wide), 0)
        q = lax.broadcasted_iota(jnp.int32, (high, wide), 1)
        inside = (
            ((p >= margin) | (flag_ref[4:5, :wide] == 0.0))
            & ((p < margin + tile_rows) | (flag_ref[5:6, :wide] == 0.0))
            & ((q >= reach) | (follows[:, :wide] > 0.0))
            & (q < reach + tile_cols)
        )
        seen = jnp.zeros((tile_rows, tile_cols), f32)
        for n in range(n_img):
            total = jnp.concatenate(
                [
                    before_ref[:, n * 2 * reach : (n + 1) * 2 * reach],
                    jnp.zeros((high, wide - 2 * reach), f32),
                ],
                axis=1,
            ) + jnp.concatenate(
                [jnp.zeros((high, reach), f32), part_ref[n], jnp.zeros((high, wide - reach - tile_cols), f32)],
                axis=1,
            )
            recon = (total + flag_ref[6:7, :wide]).astype(bf16).astype(f32)
            img_ref[n] = jnp.where(inside, recon, 0.0)
            mine = img_ref[n, margin : margin + tile_rows, reach : reach + tile_cols]
            recon_ref[n] = mine.astype(bf16)
            seen = seen + (vis_ref[n].astype(f32) - mine)
        seen = jnp.sum(seen, keepdims=True)
        patches(img_ref, col_ref, tile_rows)
        a = col_ref[...].astype(bf16)
        a2_ref[:rows, :] = a_ref[...]
        a2_ref[rows:, :] = -a
        p2_ref[:rows, :] = prob_ref[...]
        hidden = jnp.zeros((1, LANES), f32)
        for v in range(chunks):
            at = slice(v * LANES, (v + 1) * LANES)
            act = jnp.dot(a, w_ref[:, at], preferred_element_type=f32) + bias_ref[...]
            lift = jnp.exp(act)
            prob = lift / (1.0 + block_sum(lift))
            if v < edge:
                prob = jnp.where(follows > 0.0, prob, 0.0)
            if v >= chunks - edge:
                prob = jnp.where(ends > 0.0, prob, 0.0)
            p2_ref[rows:, at] = prob.astype(bf16)
            hidden = hidden + (hid_ref[:, at] - jnp.sum(prob, axis=0, keepdims=True))
        g_ref[...] = lax.dot_general(
            a2_ref[...], p2_ref[...], (((0,), (0,)), ((), ())), preferred_element_type=f32
        )
        lane = lax.broadcasted_iota(jnp.int32, (side, LANES), 1)
        cmb_ref[...] = jnp.zeros_like(cmb_ref)
        for r in range(side):
            acc = g_ref[pl.ds(r * wide, side + 1), pl.ds(0, LANES)]
            for v in range(1, chunks):
                acc = acc + g_ref[pl.ds(r * wide + 2 * v, side + 1), pl.ds(v * LANES, LANES)]
            half = pltpu.roll(acc, channels, 1)
            cmb_ref[r * side : (r + 1) * side, :] = jnp.where(
                lane < channels, acc[:side] + half[1 : side + 1], half[:side] + acc[1 : side + 1]
            )
        hidden = hidden + pltpu.roll(hidden, channels, 1)
        lane = lax.broadcasted_iota(jnp.int32, (quarter, LANES), 1)
        sum_ref[...] = jnp.zeros_like(sum_ref)
        for half, last in ((0, hidden), (1, jnp.broadcast_to(seen, (1, LANES)))):
            at, to = 2 * half * quarter, half * half_rows
            sum_ref[to : to + quarter, :] = jnp.where(
                lane < channels, cmb_ref[at : at + quarter, :], cmb_ref[at + quarter : at + 2 * quarter, :]
            )
            sum_ref[to + quarter : to + quarter + 1, :] = last
        sent(sum_ref, pack_ref)

    def sent(sum_ref, pack_ref):
        for half in range(2):
            at = half * half_rows + quarter
            last = sum_ref[at : at + 1, :]
            sum_ref[at + 1 : at + 2, :] = last - last.astype(bf16).astype(f32)
        packed = sum_ref[...].astype(bf16)
        for to in range(pack_ref.shape[0]):
            pack_ref[to] = packed

    def added(parts_ref, sum_ref):
        sum_ref[...] = jnp.sum(parts_ref[...].astype(f32), axis=0)
        for half in range(2):
            at = half * half_rows + quarter
            sum_ref[at : at + 1, :] += sum_ref[at + 1 : at + 2, :]

    def spread_kernel(parts_ref, pack_ref, sum_ref):
        added(parts_ref, sum_ref)
        sent(sum_ref, pack_ref)

    def finish_kernel(parts_ref, recon_in_ref, recon_ref, grad_ref, hid_ref, seen_ref, sum_ref, flat_ref):
        recon_ref[...] = recon_in_ref[...]
        added(parts_ref, sum_ref)
        sum_ref[...] = sum_ref[...] * scale
        for part in range(4):
            at, lane = part // 2 * half_rows, part % 2 * channels
            flat_ref[part * quarter : (part + 1) * quarter, :] = sum_ref[at : at + quarter, lane : lane + channels]
        for r in range(side):
            grad_ref[r] = flat_ref[r * side : (r + 1) * side, :]
        hid_ref[...] = sum_ref[quarter : quarter + 1, :channels]
        seen_ref[...] = sum_ref[half_rows + quarter : half_rows + quarter + 1, :1]

    taps_first = filters.astype(f32).transpose(1, 2, 0)
    pairs = jnp.concatenate(
        [jnp.pad(taps_first, ((0, 0), (0, 1), (0, 0))), jnp.pad(taps_first, ((0, 0), (1, 0), (0, 0)))],
        axis=2,
    )
    bias = jnp.concatenate([hidden_bias, hidden_bias])[None]
    col_at, row_at = lax.axis_index(COL), lax.axis_index(ROW)
    first, last = col_at == 0, col_at == lax.axis_size(COL) - 1
    top, bottom = row_at == 0, row_at == lax.axis_size(ROW) - 1
    line = lax.broadcasted_iota(jnp.int32, (8, LANES), 0)
    flags = jnp.zeros((8, LANES), f32)
    for at, value in enumerate(
        (first, ~first, last, ~last, top, bottom, visible_unit_bias)
    ):
        flags = jnp.where(line == at, jnp.asarray(value, f32), flags)

    payload = shape((n_img, reach, own + 2 * tile_cols), bf16)
    downward, upward = call(
        pack_kernel,
        (payload, payload),
        [pltpu.VMEM(images.shape, bf16), pltpu.SemaphoreType.DMA((3,))],
        "pack",
        left=(0, 1),
    )(in_hbm(images), in_hbm(unit_noise))
    before, after = edges(ROW, downward, upward)
    (w,) = call(
        band_kernel, (shape((taps, units), bf16),), [pltpu.VMEM((taps, units), f32)], "band"
    )(pairs)
    column, leftward = call(
        mid_kernel,
        (shape((n_img, taller, tile_cols), bf16), shape((n_img, tall + reach, extra), bf16)),
        [pltpu.VMEM((taller, tile_cols), f32)],
        "mid",
    )(images, unit_noise, before, after)

    steps = lax.axis_size(COL) - 1
    beyond = lax.ppermute(leftward, COL, [(i + 1, i) for i in range(steps)])
    (t,) = call(draw_kernel, (shape((n_img, tall, own), f32),), [], "draw")(unit_noise, before, after)
    part, rightward, prob, a, hid = call(
        up_kernel,
        (
            shape((n_img, high, tile_cols), f32),
            shape((high, n_img * 2 * reach), f32),
            shape((rows, units), bf16),
            shape((rows, taps), bf16),
            shape((1, units), f32),
        ),
        [
            pltpu.VMEM((n_img, taller, wide), f32),
            pltpu.VMEM((n_img * tall, taps), f32),
            pltpu.VMEM((n_img * tall, units), bf16),
            pltpu.VMEM((n_img * tall, taps), f32),
        ],
        "up",
    )(flags, column, beyond, w, t, bias)

    shares = lax.ppermute(rightward, COL, [(i, i + 1) for i in range(steps)])
    sizes = [lax.axis_size(axes) for axes in GROUPS]
    recon, pack = call(
        down_kernel,
        (shape(images.shape, bf16), shape((sizes[0], part_rows, LANES), bf16)),
        [
            pltpu.VMEM((n_img, high, wide), f32),
            pltpu.VMEM((rows, taps), f32),
            pltpu.VMEM((2 * rows, taps), bf16),
            pltpu.VMEM((2 * rows, units), bf16),
            pltpu.VMEM((taps, units), f32),
            pltpu.VMEM((4 * quarter, LANES), f32),
            pltpu.VMEM((part_rows, LANES), f32),
        ],
        "down",
    )(flags, part, shares, images, w, bias, prob, a, hid)

    scratch = [pltpu.VMEM((part_rows, LANES), f32)]
    for axes, following in zip(GROUPS, sizes[1:] + [None]):
        parts = lax.all_to_all(pack, axes, 0, 0, tiled=True)
        if following:
            (pack,) = call(
                spread_kernel, (shape((following, part_rows, LANES), bf16),), scratch, "spread"
            )(parts)
    recon, grad, hidden, seen = call(
        finish_kernel,
        (
            shape(images.shape, bf16),
            shape((side, side, channels), f32),
            shape((1, channels), f32),
            shape((1, 1), f32),
        ),
        scratch + [pltpu.VMEM((4 * quarter, channels), f32)],
        "finish",
    )(parts, recon)
    return (recon, grad.transpose(2, 0, 1), hidden[0], seen[0, 0])


def solution(mesh):
    split = Mesh(
        mesh.devices.reshape(mesh.shape["img"], 2, 4, 4, 8),
        ("img", "row_0", "row_1", "col_0", "col_1"),
    )
    placed = (P("img", ROW, COL), P(), P(), P(), P("img", ROW, COL))
    return jax.shard_map(
        body,
        mesh=split,
        in_specs=placed,
        out_specs=(P("img", ROW, COL), P(), P(), P()),
        check_vma=False,
    )
```

```python
import jax
import jax.numpy as jnp
from jax import lax
from jax.experimental import pallas as pl
from jax.experimental.pallas import tpu as pltpu
from jax.sharding import Mesh
from jax.sharding import PartitionSpec as P

ROW = ("row_0", "row_1")
COL = ("col_0", "col_1", "col_2", "col_3")
LANES = 128
GROUPS = (("img", "row_1"), ("col_3", "col_2", "col_1"), ("row_0", "col_0"))
INTERPRET = False
SMALL = 0.0625
GRANT = 8 << 20


def call(kernel, out_shape, scratch, name, left=()):
    outs = out_shape if isinstance(out_shape, (list, tuple)) else (out_shape,)

    def run(*args):
        specs = [
            pl.BlockSpec(memory_space=pltpu.HBM if at in left else pltpu.VMEM)
            for at in range(len(args))
        ]
        return pl.pallas_call(
            kernel,
            out_shape=out_shape,
            in_specs=specs,
            out_specs=tuple(pl.BlockSpec(memory_space=pltpu.VMEM) for _ in outs),
            scratch_shapes=scratch,
            compiler_params=pltpu.CompilerParams(vmem_limit_bytes=GRANT),
            name=name,
            interpret=INTERPRET,
        )(*args)

    return run


def skipping(ref, lead, start, size):
    if INTERPRET:
        return ref[lead][start : start + 2 * size - 1 : 2]
    return ref[lead, pl.ds(start, size, 2), :]


def put_skipping(ref, lead, start, value):
    if INTERPRET:
        for at in range(value.shape[0]):
            ref[lead, start + 2 * at, :] = value[at]
    else:
        ref[lead, pl.ds(start, value.shape[0], 2), :] = value


def in_hbm(x):
    return x if INTERPRET else pltpu.with_memory_space_constraint(x, pltpu.HBM)


def edges(axis, tail, head):
    count = lax.axis_size(axis)
    ends = count - 1
    return (
        lax.ppermute(tail, axis, [(i, (i + 1) % count) for i in range(ends)]),
        lax.ppermute(head, axis, [((i + 1) % count, i) for i in range(ends)]),
    )


def body(images, filters, hidden_bias, visible_unit_bias, unit_noise):
    n_img, tile_rows, tile_cols = images.shape
    channels, side, _ = filters.shape
    margin = side // 2
    reach = 2 * margin
    far = 3 * margin
    high, wide = tile_rows + 2 * margin, tile_cols + 2 * margin
    tall, taller = tile_rows + 2 * reach, tile_rows + 2 * far
    broad = tile_cols + 2 * far
    rows, every = n_img * tile_rows, n_img * tall
    own, part = tile_cols * channels, reach * channels
    taps = side * wide
    chunks, edge = own // LANES, part // LANES
    few, some = tile_rows // 2, reach // 2
    count = side * side
    quarter = -(-count // 4)
    half_rows = -(-(quarter + 2) // 8) * 8
    part_rows = 2 * half_rows
    f32, bf16 = jnp.float32, jnp.bfloat16
    shape = jax.ShapeDtypeStruct
    scale = 1.0 / float(
        rows * tile_cols * lax.axis_size("img") * lax.axis_size(ROW) * lax.axis_size(COL)
    )

    def slots(odd, n):
        at = odd * (every // 2)
        beyond = at + n_img * few + n * reach
        return at + n * few, beyond, beyond + some

    def windows(ref, n, row, size, left):
        return jnp.concatenate(
            [skipping(ref, n, row + r, size)[:, left : left + wide] for r in range(side)], axis=1
        )

    def pack_kernel(vis_hbm, noise_hbm, down_ref, up_ref, vis_ref, sems):
        moves = [
            pltpu.make_async_copy(vis_hbm, vis_ref, sems.at[0]),
            pltpu.make_async_copy(
                noise_hbm.at[:, pl.ds(tile_rows - reach, reach), :], down_ref.at[:, :, pl.ds(0, own)], sems.at[1]
            ),
            pltpu.make_async_copy(
                noise_hbm.at[:, pl.ds(0, reach), :], up_ref.at[:, :, pl.ds(0, own)], sems.at[2]
            ),
        ]
        for move in moves:
            move.start()
        moves[0].wait()

        def beside(first, last, size):
            more = jnp.concatenate([last, jnp.zeros((size - last.shape[0], tile_cols), f32)], axis=0)
            return jnp.concatenate([first, more], axis=1).astype(bf16)

        for n in range(n_img):
            pixels = vis_ref[n].astype(f32)
            lowest = pixels[tile_rows - far :]
            down_ref[n, :, own:] = beside(lowest[:reach], lowest[reach:], reach)
            up_ref[n, :, own:] = beside(pixels[:reach], pixels[reach:far], reach)
        for move in moves[1:]:
            move.wait()

    def mid_kernel(vis_ref, noise_ref, before_ref, after_ref, column_ref, left_ref, right_ref):
        firsts, lasts = [], []
        for n in range(n_img):
            for at, payload in ((0, before_ref), (far + tile_rows, after_ref)):
                pixels = payload[n, :, own:].astype(f32)
                column_ref[n, at : at + reach, :] = pixels[:, :tile_cols]
                column_ref[n, at + reach : at + far, :] = pixels[: far - reach, tile_cols:]
            column_ref[n, far : far + tile_rows, :] = vis_ref[n].astype(f32)
            for ref, lane in ((left_ref, 0), (right_ref, own - part)):
                at = n * tall
                ref[at : at + reach, :] = before_ref[n, :, lane : lane + part]
                ref[at + reach : at + reach + tile_rows, :] = noise_ref[n, :, lane : lane + part]
                ref[at + reach + tile_rows : at + tall, :] = after_ref[n, :, lane : lane + part]
            for at in range(0, taller, reach):
                block = column_ref[n, at : at + reach, :]
                firsts.append(block[:, :far])
                lasts.append(block[:, tile_cols - far :])
        for ref, blocks in ((left_ref, firsts), (right_ref, lasts)):
            gap = jnp.zeros((reach, part - len(blocks) * far), f32)
            ref[every:, :] = jnp.concatenate(blocks + [gap], axis=1).astype(bf16)

    def band_kernel(pair_ref, w_ref, wide_ref):
        wide_ref[...] = jnp.zeros_like(wide_ref)
        for r in range(side):
            block = pair_ref[r]
            for v in range(chunks):
                wide_ref[pl.ds(r * wide + 2 * v, side + 1), pl.ds(v * LANES, LANES)] = block
        w_ref[...] = wide_ref[...].astype(bf16)

    def inverse(u):
        u = u.astype(f32)
        return jnp.where(u > 0.0, 1.0 / jnp.log(u), 0.0)

    def placed(tmp_ref, out_ref, n, lane):
        for odd in range(2):
            mine, above, below = slots(odd, n)
            for v in range(tmp_ref.shape[0]):
                lanes = slice(lane + v * LANES, lane + (v + 1) * LANES)
                line = skipping(tmp_ref, v, odd, tall // 2)
                out_ref[above : above + some, lanes] = line[:some]
                out_ref[mine : mine + few, lanes] = line[some : some + few]
                out_ref[below : below + some, lanes] = line[some + few :]

    def draw_kernel(noise_ref, before_ref, after_ref, t_ref, tmp_ref):
        for n in range(n_img):
            for v in range(chunks):
                at = slice(v * LANES, (v + 1) * LANES)
                tmp_ref[v, :reach, :] = inverse(before_ref[n, :, at])
                tmp_ref[v, reach : reach + tile_rows, :] = inverse(noise_ref[n, :, at])
                tmp_ref[v, reach + tile_rows :, :] = inverse(after_ref[n, :, at])
            placed(tmp_ref, t_ref, n, 0)

    def odds(even, odd):
        even, odd = even * SMALL, odd * SMALL
        total = even + odd
        total = total + pltpu.roll(total, channels, 1)
        share = 1.0 / (SMALL + total)
        return even * share, odd * share

    def main_kernel(
        flag_ref, column_ref, before_ref, after_ref, w_ref, t_ref, bias_ref, vis_ref,
        recon_ref, pack_ref,
        img_ref, col_ref, samp_ref, edge_ref, tmp_ref, back_ref, a2_ref, p2_ref, g_ref, cmb_ref, sum_ref,
    ):
        half = every // 2
        mine = n_img * few
        for n in range(n_img):
            strips = []
            for ref in (before_ref, after_ref):
                at = n * (taller // reach) * far
                strips.append(
                    jnp.concatenate(
                        [
                            ref[every:, at + k * far : at + (k + 1) * far].astype(f32)
                            for k in range(taller // reach)
                        ],
                        axis=0,
                    )
                )
            img_ref[n, :, :broad] = jnp.concatenate([strips[0], column_ref[n], strips[1]], axis=1)
        for at, ref in ((0, before_ref), (1, after_ref)):
            for n in range(n_img):
                for v in range(edge):
                    tmp_ref[v] = inverse(ref[n * tall : (n + 1) * tall, v * LANES : (v + 1) * LANES])
                placed(tmp_ref, edge_ref, n, at * part)
        hidden = jnp.zeros((1, LANES), f32)
        for block in range(2):
            for odd in range(2):
                for n in range(n_img):
                    own_at, above, below = slots(odd, n)
                    line = windows(img_ref, n, odd, tall // 2, block * tile_cols)
                    col_ref[above : above + some, :] = line[:some]
                    col_ref[own_at : own_at + few, :] = line[some : some + few]
                    col_ref[below : below + some, :] = line[some + few :]
            a = col_ref[...].astype(bf16)
            for v in range(chunks):
                at = slice(v * LANES, (v + 1) * LANES)
                act = jnp.dot(a, w_ref[:, at], preferred_element_type=f32) + bias_ref[...]
                lift = jnp.exp(act)
                first, second = lift[:half], lift[half:]
                inner = v >= edge if block == 0 else v < edge
                if inner:
                    to = (v - edge if block == 0 else v + edge) * LANES
                    probs = odds(first[:mine], second[:mine])
                    for odd in range(2):
                        p2_ref[odd * mine : (odd + 1) * mine, to : to + LANES] = probs[odd].astype(bf16)
                        hidden = hidden + jnp.sum(probs[odd], axis=0, keepdims=True)
                    t = t_ref[:, to : to + LANES]
                else:
                    to = (v if block == 0 else v) * LANES
                    t = edge_ref[:, to : to + LANES]
                cold = jnp.where(t == 0.0, 0.0, lift * t)
                cold = cold * cold
                samples = odds(cold[:half], cold[half:])
                for odd in range(2):
                    at_row = block * every + odd * half
                    samp_ref[at_row : at_row + half, at] = samples[odd].astype(bf16)
        for odd in range(2):
            for n in range(n_img):
                at = (odd * n_img + n) * few
                a2_ref[at : at + few, :] = windows(img_ref, n, reach + odd, few, reach).astype(bf16)

        down = lax.dot_general(
            samp_ref[...], w_ref[...], (((1,), (1,)), ((), ())), preferred_element_type=f32
        )
        down = jnp.concatenate([down, jnp.zeros((2 * every, -taps % LANES), f32)], axis=1)
        for block in range(2):
            for odd in range(2):
                for n in range(n_img):
                    own_at, above, below = (block * every + at for at in slots(odd, n))
                    to = (block * n_img + n) * tall
                    line = jnp.concatenate(
                        [down[above : above + some], down[own_at : own_at + few], down[below : below + some]], axis=0
                    )
                    for v in range(back_ref.shape[0]):
                        put_skipping(back_ref, v, to + odd, line[:, v * LANES : (v + 1) * LANES])
        p = lax.broadcasted_iota(jnp.int32, (high, wide), 0)
        q = lax.broadcasted_iota(jnp.int32, (high, wide), 1)
        inside = (
            ((p >= margin) | (flag_ref[2:3, :wide] == 0.0))
            & ((p < margin + tile_rows) | (flag_ref[3:4, :wide] == 0.0))
            & ((q >= margin) | (flag_ref[0:1, :wide] == 0.0))
            & ((q < margin + tile_cols) | (flag_ref[1:2, :wide] == 0.0))
        )
        seen = jnp.zeros((tile_rows, tile_cols), f32)
        gap = jnp.zeros((high, reach), f32)
        for n in range(n_img):
            totals = []
            for block in range(2):
                total = jnp.zeros((high, wide), f32)
                for r in range(side):
                    at = (block * n_img + n) * tall + reach - r
                    lane, over = r * wide, max((r + 1) * wide - LANES, 0)
                    if lane < LANES < lane + wide:
                        piece = jnp.concatenate(
                            [back_ref[0, at : at + high, lane:], back_ref[1, at : at + high, :over]], axis=1
                        )
                    else:
                        lane %= LANES
                        piece = back_ref[int(over > 0), at : at + high, lane : lane + wide]
                    total = total + piece
                totals.append(total)
            total = jnp.concatenate([totals[0][:, reach:], gap], axis=1) + jnp.concatenate(
                [gap, totals[1][:, : wide - reach]], axis=1
            )
            recon = (total + flag_ref[4:5, :wide]).astype(bf16).astype(f32)
            img_ref[n, :high, :wide] = jnp.where(inside, recon, 0.0)
            middle = img_ref[n, margin : margin + tile_rows, margin : margin + tile_cols]
            recon_ref[n] = middle.astype(bf16)
            seen = seen + (vis_ref[n].astype(f32) - middle)
        seen = jnp.sum(seen, keepdims=True)

        for odd in range(2):
            for n in range(n_img):
                at = (odd * n_img + n) * few
                col_ref[at : at + few, :] = windows(img_ref, n, odd, few, 0)
        a = col_ref[:rows, :].astype(bf16)
        a2_ref[rows:, :] = -a
        for v in range(chunks):
            at = slice(v * LANES, (v + 1) * LANES)
            act = jnp.dot(a, w_ref[:, at], preferred_element_type=f32) + bias_ref[...]
            lift = jnp.exp(act)
            probs = odds(lift[:mine], lift[mine:])
            for odd in range(2):
                to = rows + odd * mine
                p2_ref[to : to + mine, at] = probs[odd].astype(bf16)
                hidden = hidden - jnp.sum(probs[odd], axis=0, keepdims=True)
        g_ref[...] = lax.dot_general(
            a2_ref[...], p2_ref[...], (((0,), (0,)), ((), ())), preferred_element_type=f32
        )
        lane = lax.broadcasted_iota(jnp.int32, (side, LANES), 1)
        cmb_ref[...] = jnp.zeros_like(cmb_ref)
        for r in range(side):
            acc = g_ref[pl.ds(r * wide, side + 1), pl.ds(0, LANES)]
            for v in range(1, chunks):
                acc = acc + g_ref[pl.ds(r * wide + 2 * v, side + 1), pl.ds(v * LANES, LANES)]
            turned = pltpu.roll(acc, channels, 1)
            cmb_ref[r * side : (r + 1) * side, :] = jnp.where(
                lane < channels, acc[:side] + turned[1 : side + 1], turned[:side] + acc[1 : side + 1]
            )
        hidden = hidden + pltpu.roll(hidden, channels, 1)
        lane = lax.broadcasted_iota(jnp.int32, (quarter, LANES), 1)
        sum_ref[...] = jnp.zeros_like(sum_ref)
        for half, last in ((0, hidden), (1, jnp.broadcast_to(seen, (1, LANES)))):
            at, to = 2 * half * quarter, half * half_rows
            sum_ref[to : to + quarter, :] = jnp.where(
                lane < channels, cmb_ref[at : at + quarter, :], cmb_ref[at + quarter : at + 2 * quarter, :]
            )
            sum_ref[to + quarter : to + quarter + 1, :] = last
        sent(sum_ref, pack_ref)

    def sent(sum_ref, pack_ref):
        for half in range(2):
            at = half * half_rows + quarter
            last = sum_ref[at : at + 1, :]
            sum_ref[at + 1 : at + 2, :] = last - last.astype(bf16).astype(f32)
        packed = sum_ref[...].astype(bf16)
        for to in range(pack_ref.shape[0]):
            pack_ref[to] = packed

    def added(parts_ref, sum_ref):
        sum_ref[...] = jnp.sum(parts_ref[...].astype(f32), axis=0)
        for half in range(2):
            at = half * half_rows + quarter
            sum_ref[at : at + 1, :] += sum_ref[at + 1 : at + 2, :]

    def spread_kernel(parts_ref, pack_ref, sum_ref):
        added(parts_ref, sum_ref)
        sent(sum_ref, pack_ref)

    def finish_kernel(parts_ref, recon_in_ref, recon_ref, grad_ref, hid_ref, seen_ref, sum_ref, flat_ref):
        recon_ref[...] = recon_in_ref[...]
        added(parts_ref, sum_ref)
        sum_ref[...] = sum_ref[...] * scale
        for part in range(4):
            at, lane = part // 2 * half_rows, part % 2 * channels
            flat_ref[part * quarter : (part + 1) * quarter, :] = sum_ref[at : at + quarter, lane : lane + channels]
        for r in range(side):
            grad_ref[r] = flat_ref[r * side : (r + 1) * side, :]
        hid_ref[...] = sum_ref[quarter : quarter + 1, :channels]
        seen_ref[...] = sum_ref[half_rows + quarter : half_rows + quarter + 1, :1]

    taps_first = filters.astype(f32).transpose(1, 2, 0)
    pairs = jnp.concatenate(
        [jnp.pad(taps_first, ((0, 0), (0, 1), (0, 0))), jnp.pad(taps_first, ((0, 0), (1, 0), (0, 0)))],
        axis=2,
    )
    bias = jnp.concatenate([hidden_bias, hidden_bias])[None]
    col_at, row_at = lax.axis_index(COL), lax.axis_index(ROW)
    first, last = col_at == 0, col_at == lax.axis_size(COL) - 1
    top, bottom = row_at == 0, row_at == lax.axis_size(ROW) - 1
    line = lax.broadcasted_iota(jnp.int32, (8, LANES), 0)
    flags = jnp.zeros((8, LANES), f32)
    for at, value in enumerate((first, last, top, bottom, visible_unit_bias)):
        flags = jnp.where(line == at, jnp.asarray(value, f32), flags)

    payload = shape((n_img, reach, own + 2 * tile_cols), bf16)
    downward, upward = call(
        pack_kernel,
        (payload, payload),
        [pltpu.VMEM(images.shape, bf16), pltpu.SemaphoreType.DMA((3,))],
        "pack",
        left=(0, 1),
    )(in_hbm(images), in_hbm(unit_noise))
    before, after = edges(ROW, downward, upward)
    (w,) = call(
        band_kernel, (shape((taps, own), bf16),), [pltpu.VMEM((taps, own), f32)], "band"
    )(pairs)
    sideways = shape((every + reach, part), bf16)
    column, leftward, rightward = call(
        mid_kernel, (shape((n_img, taller, tile_cols), f32), sideways, sideways), [], "mid"
    )(images, unit_noise, before, after)

    left, right = edges(COL, rightward, leftward)
    (t,) = call(
        draw_kernel, (shape((every, own), f32),), [pltpu.VMEM((chunks, tall, LANES), f32)], "draw"
    )(unit_noise, before, after)
    sizes = [lax.axis_size(axes) for axes in GROUPS]
    recon, pack = call(
        main_kernel,
        (shape(images.shape, bf16), shape((sizes[0], part_rows, LANES), bf16)),
        [
            pltpu.VMEM((n_img, taller, LANES), f32),
            pltpu.VMEM((every, taps), f32),
            pltpu.VMEM((2 * every, own), bf16),
            pltpu.VMEM((every, 2 * part), f32),
            pltpu.VMEM((edge, tall, LANES), f32),
            pltpu.VMEM((-(-taps // LANES), 2 * every, LANES), f32),
            pltpu.VMEM((2 * rows, taps), bf16),
            pltpu.VMEM((2 * rows, own), bf16),
            pltpu.VMEM((taps, own), f32),
            pltpu.VMEM((4 * quarter, LANES), f32),
            pltpu.VMEM((part_rows, LANES), f32),
        ],
        "main",
    )(flags, column, left, right, w, t, bias, images)

    scratch = [pltpu.VMEM((part_rows, LANES), f32)]
    for axes, following in zip(GROUPS, sizes[1:] + [None]):
        parts = lax.all_to_all(pack, axes, 0, 0, tiled=True)
        if following:
            (pack,) = call(
                spread_kernel, (shape((following, part_rows, LANES), bf16),), scratch, "spread"
            )(parts)
    recon, grad, hidden, seen = call(
        finish_kernel,
        (
            shape(images.shape, bf16),
            shape((side, side, channels), f32),
            shape((1, channels), f32),
            shape((1, 1), f32),
        ),
        scratch + [pltpu.VMEM((4 * quarter, channels), f32)],
        "finish",
    )(parts, recon)
    return (recon, grad.transpose(2, 0, 1), hidden[0], seen[0, 0])


def solution(mesh):
    split = Mesh(
        mesh.devices.reshape(mesh.shape["img"], 2, 4, 4, 2, 2, 2),
        ("img",) + ROW + COL,
    )
    placed = (P("img", ROW, COL), P(), P(), P(), P("img", ROW, COL))
    return jax.shard_map(
        body,
        mesh=split,
        in_specs=placed,
        out_specs=(P("img", ROW, COL), P(), P(), P()),
        check_vma=False,
    )
```

```python
import jax
import jax.numpy as jnp
from jax import lax
from jax.experimental import pallas as pl
from jax.experimental.pallas import tpu as pltpu
from jax.sharding import Mesh
from jax.sharding import PartitionSpec as P

ROW = ("row_0", "row_1")
COL = ("col_0", "col_1", "col_2", "col_3")
LANES = 128
GROUPS = (("img", "row_1"), ("row_0", "col_0"), ("col_3", "col_2", "col_1"))
INTERPRET = False
SMALL = 0.0625
GRANT = 8 << 20


def call(kernel, out_shape, scratch, name, left=()):
    outs = out_shape if isinstance(out_shape, (list, tuple)) else (out_shape,)

    def run(*args):
        specs = [
            pl.BlockSpec(memory_space=pltpu.HBM if at in left else pltpu.VMEM)
            for at in range(len(args))
        ]
        return pl.pallas_call(
            kernel,
            out_shape=out_shape,
            in_specs=specs,
            out_specs=tuple(pl.BlockSpec(memory_space=pltpu.VMEM) for _ in outs),
            scratch_shapes=scratch,
            compiler_params=pltpu.CompilerParams(vmem_limit_bytes=GRANT),
            name=name,
            interpret=INTERPRET,
        )(*args)

    return run


def skipping(ref, lead, start, size):
    if INTERPRET:
        return ref[lead][start : start + 2 * size - 1 : 2]
    return ref[lead, pl.ds(start, size, 2), :]


def put_skipping(ref, lead, start, value):
    if INTERPRET:
        for at in range(value.shape[0]):
            ref[lead, start + 2 * at, :] = value[at]
    else:
        ref[lead, pl.ds(start, value.shape[0], 2), :] = value


def in_hbm(x):
    return x if INTERPRET else pltpu.with_memory_space_constraint(x, pltpu.HBM)


def edges(axis, tail, head):
    count = lax.axis_size(axis)
    ends = count - 1
    return (
        lax.ppermute(tail, axis, [(i, (i + 1) % count) for i in range(ends)]),
        lax.ppermute(head, axis, [((i + 1) % count, i) for i in range(ends)]),
    )


def body(images, filters, hidden_bias, visible_unit_bias, unit_noise):
    n_img, tile_rows, tile_cols = images.shape
    channels, side, _ = filters.shape
    margin = side // 2
    reach = 2 * margin
    far = 3 * margin
    high, wide = tile_rows + 2 * margin, tile_cols + 2 * margin
    tall, taller = tile_rows + 2 * reach, tile_rows + 2 * far
    broad = tile_cols + 2 * far
    rows, every = n_img * tile_rows, n_img * tall
    own, part = tile_cols * channels, reach * channels
    taps = side * wide
    chunks, edge = own // LANES, part // LANES
    few, some = tile_rows // 2, reach // 2
    count = side * side
    quarter = -(-count // 4)
    half_rows = -(-(quarter + 2) // 8) * 8
    part_rows = 2 * half_rows
    f32, bf16 = jnp.float32, jnp.bfloat16
    shape = jax.ShapeDtypeStruct
    scale = 1.0 / float(
        rows * tile_cols * lax.axis_size("img") * lax.axis_size(ROW) * lax.axis_size(COL)
    )

    def slots(odd, n):
        at = odd * (every // 2)
        beyond = at + n_img * few + n * reach
        return at + n * few, beyond, beyond + some

    def windows(ref, n, row, size, left):
        return jnp.concatenate(
            [skipping(ref, n, row + r, size)[:, left : left + wide] for r in range(side)], axis=1
        )

    def pack_kernel(vis_hbm, noise_hbm, down_ref, up_ref, vis_ref, sems):
        moves = [
            pltpu.make_async_copy(vis_hbm, vis_ref, sems.at[0]),
            pltpu.make_async_copy(
                noise_hbm.at[:, pl.ds(tile_rows - reach, reach), :], down_ref.at[:, :, pl.ds(0, own)], sems.at[1]
            ),
            pltpu.make_async_copy(
                noise_hbm.at[:, pl.ds(0, reach), :], up_ref.at[:, :, pl.ds(0, own)], sems.at[2]
            ),
        ]
        for move in moves:
            move.start()
        moves[0].wait()

        def beside(first, last, size):
            more = jnp.concatenate([last, jnp.zeros((size - last.shape[0], tile_cols), f32)], axis=0)
            return jnp.concatenate([first, more], axis=1).astype(bf16)

        for n in range(n_img):
            pixels = vis_ref[n].astype(f32)
            lowest = pixels[tile_rows - far :]
            down_ref[n, :, own:] = beside(lowest[:reach], lowest[reach:], reach)
            up_ref[n, :, own:] = beside(pixels[:reach], pixels[reach:far], reach)
        for move in moves[1:]:
            move.wait()

    def mid_kernel(vis_ref, noise_ref, before_ref, after_ref, column_ref, left_ref, right_ref):
        firsts, lasts = [], []
        for n in range(n_img):
            for at, payload in ((0, before_ref), (far + tile_rows, after_ref)):
                pixels = payload[n, :, own:].astype(f32)
                column_ref[n, at : at + reach, :] = pixels[:, :tile_cols]
                column_ref[n, at + reach : at + far, :] = pixels[: far - reach, tile_cols:]
            column_ref[n, far : far + tile_rows, :] = vis_ref[n].astype(f32)
            for ref, lane in ((left_ref, 0), (right_ref, own - part)):
                at = n * tall
                ref[at : at + reach, :] = before_ref[n, :, lane : lane + part]
                ref[at + reach : at + reach + tile_rows, :] = noise_ref[n, :, lane : lane + part]
                ref[at + reach + tile_rows : at + tall, :] = after_ref[n, :, lane : lane + part]
            for at in range(0, taller, reach):
                block = column_ref[n, at : at + reach, :]
                firsts.append(block[:, :far])
                lasts.append(block[:, tile_cols - far :])
        for ref, blocks in ((left_ref, firsts), (right_ref, lasts)):
            gap = jnp.zeros((reach, part - len(blocks) * far), f32)
            ref[every:, :] = jnp.concatenate(blocks + [gap], axis=1).astype(bf16)

    def band_kernel(pair_ref, w_ref, wide_ref):
        wide_ref[...] = jnp.zeros_like(wide_ref)
        for r in range(side):
            block = pair_ref[r]
            for v in range(chunks):
                wide_ref[pl.ds(r * wide + 2 * v, side + 1), pl.ds(v * LANES, LANES)] = block
        w_ref[...] = wide_ref[...].astype(bf16)

    def inverse(u):
        u = u.astype(f32)
        return jnp.where(u > 0.0, 1.0 / jnp.log(u), 0.0)

    def placed(tmp_ref, out_ref, n, lane):
        for odd in range(2):
            mine, above, below = slots(odd, n)
            for v in range(tmp_ref.shape[0]):
                lanes = slice(lane + v * LANES, lane + (v + 1) * LANES)
                line = skipping(tmp_ref, v, odd, tall // 2)
                out_ref[above : above + some, lanes] = line[:some]
                out_ref[mine : mine + few, lanes] = line[some : some + few]
                out_ref[below : below + some, lanes] = line[some + few :]

    def draw_kernel(noise_ref, before_ref, after_ref, t_ref, tmp_ref):
        for n in range(n_img):
            for v in range(chunks):
                at = slice(v * LANES, (v + 1) * LANES)
                tmp_ref[v, :reach, :] = inverse(before_ref[n, :, at])
                tmp_ref[v, reach : reach + tile_rows, :] = inverse(noise_ref[n, :, at])
                tmp_ref[v, reach + tile_rows :, :] = inverse(after_ref[n, :, at])
            placed(tmp_ref, t_ref, n, 0)

    def odds(even, odd):
        even, odd = even * SMALL, odd * SMALL
        total = even + odd
        total = total + pltpu.roll(total, channels, 1)
        share = 1.0 / (SMALL + total)
        return even * share, odd * share

    def main_kernel(
        flag_ref, column_ref, before_ref, after_ref, w_ref, t_ref, bias_ref, vis_ref,
        recon_ref, pack_ref,
        img_ref, col_ref, samp_ref, edge_ref, tmp_ref, back_ref, a2_ref, p2_ref, g_ref, cmb_ref, sum_ref,
    ):
        half = every // 2
        mine = n_img * few
        for n in range(n_img):
            strips = []
            for ref in (before_ref, after_ref):
                at = n * (taller // reach) * far
                strips.append(
                    jnp.concatenate(
                        [
                            ref[every:, at + k * far : at + (k + 1) * far].astype(f32)
                            for k in range(taller // reach)
                        ],
                        axis=0,
                    )
                )
            img_ref[n, :, :broad] = jnp.concatenate([strips[0], column_ref[n], strips[1]], axis=1)
        for at, ref in ((0, before_ref), (1, after_ref)):
            for n in range(n_img):
                for v in range(edge):
                    tmp_ref[v] = inverse(ref[n * tall : (n + 1) * tall, v * LANES : (v + 1) * LANES])
                placed(tmp_ref, edge_ref, n, at * part)
        hidden = jnp.zeros((1, LANES), f32)
        for block in range(2):
            for odd in range(2):
                for n in range(n_img):
                    own_at, above, below = slots(odd, n)
                    line = windows(img_ref, n, odd, tall // 2, block * tile_cols)
                    col_ref[above : above + some, :] = line[:some]
                    col_ref[own_at : own_at + few, :] = line[some : some + few]
                    col_ref[below : below + some, :] = line[some + few :]
            a = col_ref[...].astype(bf16)
            for v in range(chunks):
                at = slice(v * LANES, (v + 1) * LANES)
                act = jnp.dot(a, w_ref[:, at], preferred_element_type=f32) + bias_ref[...]
                lift = jnp.exp(act)
                first, second = lift[:half], lift[half:]
                inner = v >= edge if block == 0 else v < edge
                if inner:
                    to = (v - edge if block == 0 else v + edge) * LANES
                    probs = odds(first[:mine], second[:mine])
                    for odd in range(2):
                        p2_ref[odd * mine : (odd + 1) * mine, to : to + LANES] = probs[odd].astype(bf16)
                        hidden = hidden + jnp.sum(probs[odd], axis=0, keepdims=True)
                    t = t_ref[:, to : to + LANES]
                else:
                    to = (v if block == 0 else v) * LANES
                    t = edge_ref[:, to : to + LANES]
                cold = jnp.where(t == 0.0, 0.0, lift * t)
                cold = cold * cold
                samples = odds(cold[:half], cold[half:])
                for odd in range(2):
                    at_row = block * every + odd * half
                    samp_ref[at_row : at_row + half, at] = samples[odd].astype(bf16)
        for odd in range(2):
            for n in range(n_img):
                at = (odd * n_img + n) * few
                a2_ref[at : at + few, :] = windows(img_ref, n, reach + odd, few, reach).astype(bf16)

        down = lax.dot_general(
            samp_ref[...], w_ref[...], (((1,), (1,)), ((), ())), preferred_element_type=f32
        )
        down = jnp.concatenate([down, jnp.zeros((2 * every, -taps % LANES), f32)], axis=1)
        for block in range(2):
            for odd in range(2):
                for n in range(n_img):
                    own_at, above, below = (block * every + at for at in slots(odd, n))
                    to = (block * n_img + n) * tall
                    line = jnp.concatenate(
                        [down[above : above + some], down[own_at : own_at + few], down[below : below + some]], axis=0
                    )
                    for v in range(back_ref.shape[0]):
                        put_skipping(back_ref, v, to + odd, line[:, v * LANES : (v + 1) * LANES])
        p = lax.broadcasted_iota(jnp.int32, (high, wide), 0)
        q = lax.broadcasted_iota(jnp.int32, (high, wide), 1)
        inside = (
            ((p >= margin) | (flag_ref[2:3, :wide] == 0.0))
            & ((p < margin + tile_rows) | (flag_ref[3:4, :wide] == 0.0))
            & ((q >= margin) | (flag_ref[0:1, :wide] == 0.0))
            & ((q < margin + tile_cols) | (flag_ref[1:2, :wide] == 0.0))
        )
        seen = jnp.zeros((tile_rows, tile_cols), f32)
        gap = jnp.zeros((high, reach), f32)
        for n in range(n_img):
            totals = []
            for block in range(2):
                total = jnp.zeros((high, wide), f32)
                for r in range(side):
                    at = (block * n_img + n) * tall + reach - r
                    lane, over = r * wide, max((r + 1) * wide - LANES, 0)
                    if lane < LANES < lane + wide:
                        piece = jnp.concatenate(
                            [back_ref[0, at : at + high, lane:], back_ref[1, at : at + high, :over]], axis=1
                        )
                    else:
                        lane %= LANES
                        piece = back_ref[int(over > 0), at : at + high, lane : lane + wide]
                    total = total + piece
                totals.append(total)
            total = jnp.concatenate([totals[0][:, reach:], gap], axis=1) + jnp.concatenate(
                [gap, totals[1][:, : wide - reach]], axis=1
            )
            recon = (total + flag_ref[4:5, :wide]).astype(bf16).astype(f32)
            img_ref[n, :high, :wide] = jnp.where(inside, recon, 0.0)
            middle = img_ref[n, margin : margin + tile_rows, margin : margin + tile_cols]
            recon_ref[n] = middle.astype(bf16)
            seen = seen + (vis_ref[n].astype(f32) - middle)
        seen = jnp.sum(seen, keepdims=True)

        for odd in range(2):
            for n in range(n_img):
                at = (odd * n_img + n) * few
                col_ref[at : at + few, :] = windows(img_ref, n, odd, few, 0)
        a = col_ref[:rows, :].astype(bf16)
        a2_ref[rows:, :] = -a
        for v in range(chunks):
            at = slice(v * LANES, (v + 1) * LANES)
            act = jnp.dot(a, w_ref[:, at], preferred_element_type=f32) + bias_ref[...]
            lift = jnp.exp(act)
            probs = odds(lift[:mine], lift[mine:])
            for odd in range(2):
                to = rows + odd * mine
                p2_ref[to : to + mine, at] = probs[odd].astype(bf16)
                hidden = hidden - jnp.sum(probs[odd], axis=0, keepdims=True)
        g_ref[...] = lax.dot_general(
            a2_ref[...], p2_ref[...], (((0,), (0,)), ((), ())), preferred_element_type=f32
        )
        lane = lax.broadcasted_iota(jnp.int32, (side, LANES), 1)
        cmb_ref[...] = jnp.zeros_like(cmb_ref)
        for r in range(side):
            acc = g_ref[pl.ds(r * wide, side + 1), pl.ds(0, LANES)]
            for v in range(1, chunks):
                acc = acc + g_ref[pl.ds(r * wide + 2 * v, side + 1), pl.ds(v * LANES, LANES)]
            turned = pltpu.roll(acc, channels, 1)
            cmb_ref[r * side : (r + 1) * side, :] = jnp.where(
                lane < channels, acc[:side] + turned[1 : side + 1], turned[:side] + acc[1 : side + 1]
            )
        hidden = hidden + pltpu.roll(hidden, channels, 1)
        lane = lax.broadcasted_iota(jnp.int32, (quarter, LANES), 1)
        sum_ref[...] = jnp.zeros_like(sum_ref)
        for half, last in ((0, hidden), (1, jnp.broadcast_to(seen, (1, LANES)))):
            at, to = 2 * half * quarter, half * half_rows
            sum_ref[to : to + quarter, :] = jnp.where(
                lane < channels, cmb_ref[at : at + quarter, :], cmb_ref[at + quarter : at + 2 * quarter, :]
            )
            sum_ref[to + quarter : to + quarter + 1, :] = last
        sent(sum_ref, pack_ref)

    def sent(sum_ref, pack_ref):
        for half in range(2):
            at = half * half_rows + quarter
            last = sum_ref[at : at + 1, :]
            sum_ref[at + 1 : at + 2, :] = last - last.astype(bf16).astype(f32)
        packed = sum_ref[...].astype(bf16)
        for to in range(pack_ref.shape[0]):
            pack_ref[to] = packed

    def added(parts_ref, sum_ref):
        sum_ref[...] = jnp.sum(parts_ref[...].astype(f32), axis=0)
        for half in range(2):
            at = half * half_rows + quarter
            sum_ref[at : at + 1, :] += sum_ref[at + 1 : at + 2, :]

    def spread_kernel(parts_ref, pack_ref, sum_ref):
        added(parts_ref, sum_ref)
        sent(sum_ref, pack_ref)

    def finish_kernel(parts_ref, recon_in_ref, recon_ref, grad_ref, hid_ref, seen_ref, sum_ref, flat_ref):
        recon_ref[...] = recon_in_ref[...]
        added(parts_ref, sum_ref)
        sum_ref[...] = sum_ref[...] * scale
        for part in range(4):
            at, lane = part // 2 * half_rows, part % 2 * channels
            flat_ref[part * quarter : (part + 1) * quarter, :] = sum_ref[at : at + quarter, lane : lane + channels]
        for r in range(side):
            grad_ref[r] = flat_ref[r * side : (r + 1) * side, :]
        hid_ref[...] = sum_ref[quarter : quarter + 1, :channels]
        seen_ref[...] = sum_ref[half_rows + quarter : half_rows + quarter + 1, :1]

    taps_first = filters.astype(f32).transpose(1, 2, 0)
    pairs = jnp.concatenate(
        [jnp.pad(taps_first, ((0, 0), (0, 1), (0, 0))), jnp.pad(taps_first, ((0, 0), (1, 0), (0, 0)))],
        axis=2,
    )
    bias = jnp.concatenate([hidden_bias, hidden_bias])[None]
    col_at, row_at = lax.axis_index(COL), lax.axis_index(ROW)
    first, last = col_at == 0, col_at == lax.axis_size(COL) - 1
    top, bottom = row_at == 0, row_at == lax.axis_size(ROW) - 1
    line = lax.broadcasted_iota(jnp.int32, (8, LANES), 0)
    flags = jnp.zeros((8, LANES), f32)
    for at, value in enumerate((first, last, top, bottom, visible_unit_bias)):
        flags = jnp.where(line == at, jnp.asarray(value, f32), flags)

    payload = shape((n_img, reach, own + 2 * tile_cols), bf16)
    downward, upward = call(
        pack_kernel,
        (payload, payload),
        [pltpu.VMEM(images.shape, bf16), pltpu.SemaphoreType.DMA((3,))],
        "pack",
        left=(0, 1),
    )(in_hbm(images), in_hbm(unit_noise))
    before, after = edges(ROW, downward, upward)
    (w,) = call(
        band_kernel, (shape((taps, own), bf16),), [pltpu.VMEM((taps, own), f32)], "band"
    )(pairs)
    sideways = shape((every + reach, part), bf16)
    column, leftward, rightward = call(
        mid_kernel, (shape((n_img, taller, tile_cols), f32), sideways, sideways), [], "mid"
    )(images, unit_noise, before, after)

    left, right = edges(COL, rightward, leftward)
    (t,) = call(
        draw_kernel, (shape((every, own), f32),), [pltpu.VMEM((chunks, tall, LANES), f32)], "draw"
    )(unit_noise, before, after)
    sizes = [lax.axis_size(axes) for axes in GROUPS]
    recon, pack = call(
        main_kernel,
        (shape(images.shape, bf16), shape((sizes[0], part_rows, LANES), bf16)),
        [
            pltpu.VMEM((n_img, taller, LANES), f32),
            pltpu.VMEM((every, taps), f32),
            pltpu.VMEM((2 * every, own), bf16),
            pltpu.VMEM((every, 2 * part), f32),
            pltpu.VMEM((edge, tall, LANES), f32),
            pltpu.VMEM((-(-taps // LANES), 2 * every, LANES), f32),
            pltpu.VMEM((2 * rows, taps), bf16),
            pltpu.VMEM((2 * rows, own), bf16),
            pltpu.VMEM((taps, own), f32),
            pltpu.VMEM((4 * quarter, LANES), f32),
            pltpu.VMEM((part_rows, LANES), f32),
        ],
        "main",
    )(flags, column, left, right, w, t, bias, images)

    scratch = [pltpu.VMEM((part_rows, LANES), f32)]
    for axes, following in zip(GROUPS, sizes[1:] + [None]):
        parts = lax.all_to_all(pack, axes, 0, 0, tiled=True)
        if following:
            (pack,) = call(
                spread_kernel, (shape((following, part_rows, LANES), bf16),), scratch, "spread"
            )(parts)
    recon, grad, hidden, seen = call(
        finish_kernel,
        (
            shape(images.shape, bf16),
            shape((side, side, channels), f32),
            shape((1, channels), f32),
            shape((1, 1), f32),
        ),
        scratch + [pltpu.VMEM((4 * quarter, channels), f32)],
        "finish",
    )(parts, recon)
    return (recon, grad.transpose(2, 0, 1), hidden[0], seen[0, 0])


def solution(mesh):
    split = Mesh(
        mesh.devices.reshape(mesh.shape["img"], 2, 4, 4, 2, 2, 2),
        ("img",) + ROW + COL,
    )
    placed = (P("img", ROW, COL), P(), P(), P(), P("img", ROW, COL))
    return jax.shard_map(
        body,
        mesh=split,
        in_specs=placed,
        out_specs=(P("img", ROW, COL), P(), P(), P()),
        check_vma=False,
    )
```

```python
import jax
import jax.numpy as jnp
from jax import lax
from jax.experimental import pallas as pl
from jax.experimental.pallas import tpu as pltpu
from jax.sharding import Mesh
from jax.sharding import PartitionSpec as P

ROW = ("row_0", "row_1")
COL = ("col_0", "col_4", "col_1", "col_2", "col_3")
LANES = 128
GROUPS = (("img", "row_1"), ("row_0", "col_4", "col_0"), ("col_3", "col_2", "col_1"))
INTERPRET = False
SMALL = 0.0625
GRANT = 8 << 20


def call(kernel, out_shape, scratch, name, left=()):
    outs = out_shape if isinstance(out_shape, (list, tuple)) else (out_shape,)

    def run(*args):
        specs = [
            pl.BlockSpec(memory_space=pltpu.HBM if at in left else pltpu.VMEM)
            for at in range(len(args))
        ]
        return pl.pallas_call(
            kernel,
            out_shape=out_shape,
            in_specs=specs,
            out_specs=tuple(pl.BlockSpec(memory_space=pltpu.VMEM) for _ in outs),
            scratch_shapes=scratch,
            compiler_params=pltpu.CompilerParams(vmem_limit_bytes=GRANT),
            name=name,
            interpret=INTERPRET,
        )(*args)

    return run


def skipping(ref, lead, start, size):
    if INTERPRET:
        return ref[lead][start : start + 2 * size - 1 : 2]
    return ref[lead, pl.ds(start, size, 2), :]


def put_skipping(ref, lead, start, value):
    if INTERPRET:
        for at in range(value.shape[0]):
            ref[lead, start + 2 * at, :] = value[at]
    else:
        ref[lead, pl.ds(start, value.shape[0], 2), :] = value


def in_hbm(x):
    return x if INTERPRET else pltpu.with_memory_space_constraint(x, pltpu.HBM)


def edges(axis, tail, head):
    count = lax.axis_size(axis)
    ends = count - 1
    return (
        lax.ppermute(tail, axis, [(i, (i + 1) % count) for i in range(ends)]),
        lax.ppermute(head, axis, [((i + 1) % count, i) for i in range(ends)]),
    )


def body(images, filters, hidden_bias, visible_unit_bias, unit_noise):
    n_img, tile_rows, tile_cols = images.shape
    channels, side, _ = filters.shape
    margin = side // 2
    reach = 2 * margin
    far = 3 * margin
    high, wide = tile_rows + 2 * margin, tile_cols + 2 * margin
    tall, taller = tile_rows + 2 * reach, tile_rows + 2 * far
    broad = tile_cols + 2 * far
    rows, every = n_img * tile_rows, n_img * tall
    own, part = tile_cols * channels, reach * channels
    taps = side * wide
    chunks, edge = own // LANES, part // LANES
    few, some = tile_rows // 2, reach // 2
    count = side * side
    quarter = -(-count // 4)
    half_rows = -(-(quarter + 2) // 8) * 8
    part_rows = 2 * half_rows
    f32, bf16 = jnp.float32, jnp.bfloat16
    shape = jax.ShapeDtypeStruct
    scale = 1.0 / float(
        rows * tile_cols * lax.axis_size("img") * lax.axis_size(ROW) * lax.axis_size(COL)
    )

    def slots(odd, n):
        at = odd * (every // 2)
        beyond = at + n_img * few + n * reach
        return at + n * few, beyond, beyond + some

    def windows(ref, n, row, size, left):
        return jnp.concatenate(
            [skipping(ref, n, row + r, size)[:, left : left + wide] for r in range(side)], axis=1
        )

    def pack_kernel(vis_hbm, noise_hbm, down_ref, up_ref, vis_ref, sems):
        moves = [
            pltpu.make_async_copy(vis_hbm, vis_ref, sems.at[0]),
            pltpu.make_async_copy(
                noise_hbm.at[:, pl.ds(tile_rows - reach, reach), :], down_ref.at[:, :, pl.ds(0, own)], sems.at[1]
            ),
            pltpu.make_async_copy(
                noise_hbm.at[:, pl.ds(0, reach), :], up_ref.at[:, :, pl.ds(0, own)], sems.at[2]
            ),
        ]
        for move in moves:
            move.start()
        moves[0].wait()

        def beside(first, last, size):
            more = jnp.concatenate([last, jnp.zeros((size - last.shape[0], tile_cols), f32)], axis=0)
            return jnp.concatenate([first, more], axis=1).astype(bf16)

        for n in range(n_img):
            pixels = vis_ref[n].astype(f32)
            lowest = pixels[tile_rows - far :]
            down_ref[n, :, own:] = beside(lowest[:reach], lowest[reach:], reach)
            up_ref[n, :, own:] = beside(pixels[:reach], pixels[reach:far], reach)
        for move in moves[1:]:
            move.wait()

    def mid_kernel(vis_ref, noise_ref, before_ref, after_ref, column_ref, left_ref, right_ref):
        firsts, lasts = [], []
        for n in range(n_img):
            for at, payload in ((0, before_ref), (far + tile_rows, after_ref)):
                pixels = payload[n, :, own:].astype(f32)
                column_ref[n, at : at + reach, :] = pixels[:, :tile_cols]
                column_ref[n, at + reach : at + far, :] = pixels[: far - reach, tile_cols:]
            column_ref[n, far : far + tile_rows, :] = vis_ref[n].astype(f32)
            for ref, lane in ((left_ref, 0), (right_ref, own - part)):
                at = n * tall
                ref[at : at + reach, :] = before_ref[n, :, lane : lane + part]
                ref[at + reach : at + reach + tile_rows, :] = noise_ref[n, :, lane : lane + part]
                ref[at + reach + tile_rows : at + tall, :] = after_ref[n, :, lane : lane + part]
            for at in range(0, taller, reach):
                block = column_ref[n, at : at + reach, :]
                firsts.append(block[:, :far])
                lasts.append(block[:, tile_cols - far :])
        for ref, blocks in ((left_ref, firsts), (right_ref, lasts)):
            gap = jnp.zeros((reach, part - len(blocks) * far), f32)
            ref[every:, :] = jnp.concatenate(blocks + [gap], axis=1).astype(bf16)

    def band_kernel(pair_ref, w_ref, wide_ref):
        wide_ref[...] = jnp.zeros_like(wide_ref)
        for r in range(side):
            block = pair_ref[r]
            for v in range(chunks):
                wide_ref[pl.ds(r * wide + 2 * v, side + 1), pl.ds(v * LANES, LANES)] = block
        w_ref[...] = wide_ref[...].astype(bf16)

    def inverse(u):
        u = u.astype(f32)
        return jnp.where(u > 0.0, 1.0 / jnp.log(u), 0.0)

    def placed(tmp_ref, out_ref, n, lane):
        for odd in range(2):
            mine, above, below = slots(odd, n)
            for v in range(tmp_ref.shape[0]):
                lanes = slice(lane + v * LANES, lane + (v + 1) * LANES)
                line = skipping(tmp_ref, v, odd, tall // 2)
                out_ref[above : above + some, lanes] = line[:some]
                out_ref[mine : mine + few, lanes] = line[some : some + few]
                out_ref[below : below + some, lanes] = line[some + few :]

    def draw_kernel(noise_ref, before_ref, after_ref, t_ref, tmp_ref):
        for n in range(n_img):
            for v in range(chunks):
                at = slice(v * LANES, (v + 1) * LANES)
                tmp_ref[v, :reach, :] = inverse(before_ref[n, :, at])
                tmp_ref[v, reach : reach + tile_rows, :] = inverse(noise_ref[n, :, at])
                tmp_ref[v, reach + tile_rows :, :] = inverse(after_ref[n, :, at])
            placed(tmp_ref, t_ref, n, 0)

    def odds(even, odd):
        even, odd = even * SMALL, odd * SMALL
        total = even + odd
        total = total + pltpu.roll(total, channels, 1)
        share = 1.0 / (SMALL + total)
        return even * share, odd * share

    def main_kernel(
        flag_ref, column_ref, before_ref, after_ref, w_ref, t_ref, bias_ref, vis_ref,
        recon_ref, pack_ref,
        img_ref, col_ref, samp_ref, edge_ref, tmp_ref, back_ref, a2_ref, p2_ref, g_ref, cmb_ref, sum_ref,
    ):
        half = every // 2
        mine = n_img * few
        for n in range(n_img):
            strips = []
            for ref in (before_ref, after_ref):
                at = n * (taller // reach) * far
                strips.append(
                    jnp.concatenate(
                        [
                            ref[every:, at + k * far : at + (k + 1) * far].astype(f32)
                            for k in range(taller // reach)
                        ],
                        axis=0,
                    )
                )
            img_ref[n, :, :broad] = jnp.concatenate([strips[0], column_ref[n], strips[1]], axis=1)
        for at, ref in ((0, before_ref), (1, after_ref)):
            for n in range(n_img):
                for v in range(edge):
                    tmp_ref[v] = inverse(ref[n * tall : (n + 1) * tall, v * LANES : (v + 1) * LANES])
                placed(tmp_ref, edge_ref, n, at * part)
        hidden = jnp.zeros((1, LANES), f32)
        for block in range(2):
            for odd in range(2):
                for n in range(n_img):
                    own_at, above, below = slots(odd, n)
                    line = windows(img_ref, n, odd, tall // 2, block * tile_cols)
                    col_ref[above : above + some, :] = line[:some]
                    col_ref[own_at : own_at + few, :] = line[some : some + few]
                    col_ref[below : below + some, :] = line[some + few :]
            a = col_ref[...].astype(bf16)
            for v in range(chunks):
                at = slice(v * LANES, (v + 1) * LANES)
                if v % 2 == 0:
                    pair = jnp.dot(a, w_ref[:, v * LANES : (v + 2) * LANES], preferred_element_type=f32)
                act = pair[:, v % 2 * LANES : (v % 2 + 1) * LANES] + bias_ref[...]
                lift = jnp.exp(act)
                first, second = lift[:half], lift[half:]
                inner = v >= edge if block == 0 else v < edge
                if inner:
                    to = (v - edge if block == 0 else v + edge) * LANES
                    probs = odds(first[:mine], second[:mine])
                    for odd in range(2):
                        p2_ref[odd * mine : (odd + 1) * mine, to : to + LANES] = probs[odd].astype(bf16)
                        hidden = hidden + jnp.sum(probs[odd], axis=0, keepdims=True)
                    t = t_ref[:, to : to + LANES]
                else:
                    to = (v if block == 0 else v) * LANES
                    t = edge_ref[:, to : to + LANES]
                cold = jnp.where(t == 0.0, 0.0, lift * t)
                cold = cold * cold
                samples = odds(cold[:half], cold[half:])
                for odd in range(2):
                    at_row = block * every + odd * half
                    samp_ref[at_row : at_row + half, at] = samples[odd].astype(bf16)
        for odd in range(2):
            for n in range(n_img):
                at = (odd * n_img + n) * few
                a2_ref[at : at + few, :] = windows(img_ref, n, reach + odd, few, reach).astype(bf16)

        down = lax.dot_general(
            samp_ref[...], w_ref[...], (((1,), (1,)), ((), ())), preferred_element_type=f32
        )
        down = jnp.concatenate([down, jnp.zeros((2 * every, -taps % LANES), f32)], axis=1)
        for block in range(2):
            for odd in range(2):
                for n in range(n_img):
                    own_at, above, below = (block * every + at for at in slots(odd, n))
                    to = (block * n_img + n) * tall
                    line = jnp.concatenate(
                        [down[above : above + some], down[own_at : own_at + few], down[below : below + some]], axis=0
                    )
                    for v in range(back_ref.shape[0]):
                        put_skipping(back_ref, v, to + odd, line[:, v * LANES : (v + 1) * LANES])
        p = lax.broadcasted_iota(jnp.int32, (high, wide), 0)
        q = lax.broadcasted_iota(jnp.int32, (high, wide), 1)
        inside = (
            ((p >= margin) | (flag_ref[2:3, :wide] == 0.0))
            & ((p < margin + tile_rows) | (flag_ref[3:4, :wide] == 0.0))
            & ((q >= margin) | (flag_ref[0:1, :wide] == 0.0))
            & ((q < margin + tile_cols) | (flag_ref[1:2, :wide] == 0.0))
        )
        seen = jnp.zeros((tile_rows, tile_cols), f32)
        gap = jnp.zeros((high, reach), f32)
        for n in range(n_img):
            totals = []
            for block in range(2):
                total = jnp.zeros((high, wide), f32)
                for r in range(side):
                    at = (block * n_img + n) * tall + reach - r
                    lane, over = r * wide, max((r + 1) * wide - LANES, 0)
                    if lane < LANES < lane + wide:
                        piece = jnp.concatenate(
                            [back_ref[0, at : at + high, lane:], back_ref[1, at : at + high, :over]], axis=1
                        )
                    else:
                        lane %= LANES
                        piece = back_ref[int(over > 0), at : at + high, lane : lane + wide]
                    total = total + piece
                totals.append(total)
            total = jnp.concatenate([totals[0][:, reach:], gap], axis=1) + jnp.concatenate(
                [gap, totals[1][:, : wide - reach]], axis=1
            )
            recon = (total + flag_ref[4:5, :wide]).astype(bf16).astype(f32)
            img_ref[n, :high, :wide] = jnp.where(inside, recon, 0.0)
            middle = img_ref[n, margin : margin + tile_rows, margin : margin + tile_cols]
            recon_ref[n] = middle.astype(bf16)
            seen = seen + (vis_ref[n].astype(f32) - middle)
        seen = jnp.sum(seen, keepdims=True)

        for odd in range(2):
            for n in range(n_img):
                at = (odd * n_img + n) * few
                col_ref[at : at + few, :] = windows(img_ref, n, odd, few, 0)
        a = col_ref[:rows, :].astype(bf16)
        a2_ref[rows:, :] = -a
        for v in range(chunks):
            at = slice(v * LANES, (v + 1) * LANES)
            if v % 2 == 0:
                pair = jnp.dot(a, w_ref[:, v * LANES : (v + 2) * LANES], preferred_element_type=f32)
            act = pair[:, v % 2 * LANES : (v % 2 + 1) * LANES] + bias_ref[...]
            lift = jnp.exp(act)
            probs = odds(lift[:mine], lift[mine:])
            for odd in range(2):
                to = rows + odd * mine
                p2_ref[to : to + mine, at] = probs[odd].astype(bf16)
                hidden = hidden - jnp.sum(probs[odd], axis=0, keepdims=True)
        g_ref[...] = lax.dot_general(
            a2_ref[...], p2_ref[...], (((0,), (0,)), ((), ())), preferred_element_type=f32
        )
        lane = lax.broadcasted_iota(jnp.int32, (side, LANES), 1)
        cmb_ref[...] = jnp.zeros_like(cmb_ref)
        for r in range(side):
            acc = g_ref[pl.ds(r * wide, side + 1), pl.ds(0, LANES)]
            for v in range(1, chunks):
                acc = acc + g_ref[pl.ds(r * wide + 2 * v, side + 1), pl.ds(v * LANES, LANES)]
            turned = pltpu.roll(acc, channels, 1)
            cmb_ref[r * side : (r + 1) * side, :] = jnp.where(
                lane < channels, acc[:side] + turned[1 : side + 1], turned[:side] + acc[1 : side + 1]
            )
        hidden = hidden + pltpu.roll(hidden, channels, 1)
        lane = lax.broadcasted_iota(jnp.int32, (quarter, LANES), 1)
        sum_ref[...] = jnp.zeros_like(sum_ref)
        for half, last in ((0, hidden), (1, jnp.broadcast_to(seen, (1, LANES)))):
            at, to = 2 * half * quarter, half * half_rows
            sum_ref[to : to + quarter, :] = jnp.where(
                lane < channels, cmb_ref[at : at + quarter, :], cmb_ref[at + quarter : at + 2 * quarter, :]
            )
            sum_ref[to + quarter : to + quarter + 1, :] = last
        sent(sum_ref, pack_ref)

    def sent(sum_ref, pack_ref):
        for half in range(2):
            at = half * half_rows + quarter
            last = sum_ref[at : at + 1, :]
            sum_ref[at + 1 : at + 2, :] = last - last.astype(bf16).astype(f32)
        packed = sum_ref[...].astype(bf16)
        for to in range(pack_ref.shape[0]):
            pack_ref[to] = packed

    def added(parts_ref, sum_ref):
        sum_ref[...] = jnp.sum(parts_ref[...].astype(f32), axis=0)
        for half in range(2):
            at = half * half_rows + quarter
            sum_ref[at : at + 1, :] += sum_ref[at + 1 : at + 2, :]

    def spread_kernel(parts_ref, pack_ref, sum_ref):
        added(parts_ref, sum_ref)
        sent(sum_ref, pack_ref)

    def finish_kernel(parts_ref, recon_in_ref, recon_ref, grad_ref, hid_ref, seen_ref, sum_ref, flat_ref):
        recon_ref[...] = recon_in_ref[...]
        added(parts_ref, sum_ref)
        sum_ref[...] = sum_ref[...] * scale
        for part in range(4):
            at, lane = part // 2 * half_rows, part % 2 * channels
            flat_ref[part * quarter : (part + 1) * quarter, :] = sum_ref[at : at + quarter, lane : lane + channels]
        for r in range(side):
            grad_ref[r] = flat_ref[r * side : (r + 1) * side, :]
        hid_ref[...] = sum_ref[quarter : quarter + 1, :channels]
        seen_ref[...] = sum_ref[half_rows + quarter : half_rows + quarter + 1, :1]

    taps_first = filters.astype(f32).transpose(1, 2, 0)
    pairs = jnp.concatenate(
        [jnp.pad(taps_first, ((0, 0), (0, 1), (0, 0))), jnp.pad(taps_first, ((0, 0), (1, 0), (0, 0)))],
        axis=2,
    )
    bias = jnp.concatenate([hidden_bias, hidden_bias])[None]
    col_at, row_at = lax.axis_index(COL), lax.axis_index(ROW)
    first, last = col_at == 0, col_at == lax.axis_size(COL) - 1
    top, bottom = row_at == 0, row_at == lax.axis_size(ROW) - 1
    line = lax.broadcasted_iota(jnp.int32, (8, LANES), 0)
    flags = jnp.zeros((8, LANES), f32)
    for at, value in enumerate((first, last, top, bottom, visible_unit_bias)):
        flags = jnp.where(line == at, jnp.asarray(value, f32), flags)

    payload = shape((n_img, reach, own + 2 * tile_cols), bf16)
    downward, upward = call(
        pack_kernel,
        (payload, payload),
        [pltpu.VMEM(images.shape, bf16), pltpu.SemaphoreType.DMA((3,))],
        "pack",
        left=(0, 1),
    )(in_hbm(images), in_hbm(unit_noise))
    before, after = edges(ROW, downward, upward)
    (w,) = call(
        band_kernel, (shape((taps, own), bf16),), [pltpu.VMEM((taps, own), f32)], "band"
    )(pairs)
    sideways = shape((every + reach, part), bf16)
    column, leftward, rightward = call(
        mid_kernel, (shape((n_img, taller, tile_cols), f32), sideways, sideways), [], "mid"
    )(images, unit_noise, before, after)

    left, right = edges(COL, rightward, leftward)
    (t,) = call(
        draw_kernel, (shape((every, own), f32),), [pltpu.VMEM((chunks, tall, LANES), f32)], "draw"
    )(unit_noise, before, after)
    sizes = [lax.axis_size(axes) for axes in GROUPS]
    recon, pack = call(
        main_kernel,
        (shape(images.shape, bf16), shape((sizes[0], part_rows, LANES), bf16)),
        [
            pltpu.VMEM((n_img, taller, LANES), f32),
            pltpu.VMEM((every, taps), f32),
            pltpu.VMEM((2 * every, own), bf16),
            pltpu.VMEM((every, 2 * part), f32),
            pltpu.VMEM((edge, tall, LANES), f32),
            pltpu.VMEM((-(-taps // LANES), 2 * every, LANES), f32),
            pltpu.VMEM((2 * rows, taps), bf16),
            pltpu.VMEM((2 * rows, own), bf16),
            pltpu.VMEM((taps, own), f32),
            pltpu.VMEM((4 * quarter, LANES), f32),
            pltpu.VMEM((part_rows, LANES), f32),
        ],
        "main",
    )(flags, column, left, right, w, t, bias, images)

    scratch = [pltpu.VMEM((part_rows, LANES), f32)]
    for axes, following in zip(GROUPS, sizes[1:] + [None]):
        parts = lax.all_to_all(pack, axes, 0, 0, tiled=True)
        if following:
            (pack,) = call(
                spread_kernel, (shape((following, part_rows, LANES), bf16),), scratch, "spread"
            )(parts)
    recon, grad, hidden, seen = call(
        finish_kernel,
        (
            shape(images.shape, bf16),
            shape((side, side, channels), f32),
            shape((1, channels), f32),
            shape((1, 1), f32),
        ),
        scratch + [pltpu.VMEM((4 * quarter, channels), f32)],
        "finish",
    )(parts, recon)
    return (recon, grad.transpose(2, 0, 1), hidden[0], seen[0, 0])


def solution(mesh):
    split = Mesh(
        mesh.devices.reshape(mesh.shape["img"], 2, 4, 2, 2, 2, 2, 2),
        ("img",) + ROW + COL,
    )
    placed = (P("img", ROW, COL), P(), P(), P(), P("img", ROW, COL))
    return jax.shard_map(
        body,
        mesh=split,
        in_specs=placed,
        out_specs=(P("img", ROW, COL), P(), P(), P()),
        check_vma=False,
    )
```

```python
import jax
import jax.numpy as jnp
from jax import lax
from jax.experimental import pallas as pl
from jax.experimental.pallas import tpu as pltpu
from jax.sharding import Mesh
from jax.sharding import PartitionSpec as P

ROW = ("row_0", "row_1")
COL = ("col_0", "col_4", "col_1", "col_2", "col_3")
LANES = 128
GROUPS = (("img", "row_1"), ("row_0", "col_4", "col_0"), ("col_3", "col_2", "col_1"))
INTERPRET = False
SMALL = 0.0625
GRANT = 8 << 20


def call(kernel, out_shape, scratch, name, left=()):
    outs = out_shape if isinstance(out_shape, (list, tuple)) else (out_shape,)

    def run(*args):
        specs = [
            pl.BlockSpec(memory_space=pltpu.HBM if at in left else pltpu.VMEM)
            for at in range(len(args))
        ]
        return pl.pallas_call(
            kernel,
            out_shape=out_shape,
            in_specs=specs,
            out_specs=tuple(pl.BlockSpec(memory_space=pltpu.VMEM) for _ in outs),
            scratch_shapes=scratch,
            compiler_params=pltpu.CompilerParams(vmem_limit_bytes=GRANT),
            name=name,
            interpret=INTERPRET,
        )(*args)

    return run


def skipping(ref, lead, start, size):
    if INTERPRET:
        return ref[lead][start : start + 2 * size - 1 : 2]
    return ref[lead, pl.ds(start, size, 2), :]


def put_skipping(ref, lead, start, value):
    if INTERPRET:
        for at in range(value.shape[0]):
            ref[lead, start + 2 * at, :] = value[at]
    else:
        ref[lead, pl.ds(start, value.shape[0], 2), :] = value


def in_hbm(x):
    return x if INTERPRET else pltpu.with_memory_space_constraint(x, pltpu.HBM)


def edges(axis, tail, head):
    count = lax.axis_size(axis)
    ends = count - 1
    after = lax.ppermute(head, axis, [((i + 1) % count, i) for i in range(ends)])
    return lax.ppermute(tail, axis, [(i, (i + 1) % count) for i in range(ends)]), after


def body(images, filters, hidden_bias, visible_unit_bias, unit_noise):
    n_img, tile_rows, tile_cols = images.shape
    channels, side, _ = filters.shape
    margin = side // 2
    reach = 2 * margin
    far = 3 * margin
    high, wide = tile_rows + 2 * margin, tile_cols + 2 * margin
    tall, taller = tile_rows + 2 * reach, tile_rows + 2 * far
    broad = tile_cols + 2 * far
    rows, every = n_img * tile_rows, n_img * tall
    own, part = tile_cols * channels, reach * channels
    taps = side * wide
    chunks, edge = own // LANES, part // LANES
    few, some = tile_rows // 2, reach // 2
    count = side * side
    quarter = -(-count // 4)
    half_rows = -(-(quarter + 2) // 8) * 8
    part_rows = 2 * half_rows
    f32, bf16 = jnp.float32, jnp.bfloat16
    shape = jax.ShapeDtypeStruct
    scale = 1.0 / float(
        rows * tile_cols * lax.axis_size("img") * lax.axis_size(ROW) * lax.axis_size(COL)
    )

    def slots(odd, n):
        at = odd * (every // 2)
        beyond = at + n_img * few + n * reach
        return at + n * few, beyond, beyond + some

    def windows(ref, n, row, size, left):
        return jnp.concatenate(
            [skipping(ref, n, row + r, size)[:, left : left + wide] for r in range(side)], axis=1
        )

    def pack_kernel(vis_hbm, noise_hbm, down_ref, up_ref, vis_ref, sems):
        moves = [
            pltpu.make_async_copy(vis_hbm, vis_ref, sems.at[0]),
            pltpu.make_async_copy(
                noise_hbm.at[:, pl.ds(tile_rows - reach, reach), :], down_ref.at[:, :, pl.ds(0, own)], sems.at[1]
            ),
            pltpu.make_async_copy(
                noise_hbm.at[:, pl.ds(0, reach), :], up_ref.at[:, :, pl.ds(0, own)], sems.at[2]
            ),
        ]
        for move in moves:
            move.start()
        moves[0].wait()

        def beside(first, last, size):
            more = jnp.concatenate([last, jnp.zeros((size - last.shape[0], tile_cols), f32)], axis=0)
            return jnp.concatenate([first, more], axis=1).astype(bf16)

        for n in range(n_img):
            pixels = vis_ref[n].astype(f32)
            lowest = pixels[tile_rows - far :]
            down_ref[n, :, own:] = beside(lowest[:reach], lowest[reach:], reach)
            up_ref[n, :, own:] = beside(pixels[:reach], pixels[reach:far], reach)
        for move in moves[1:]:
            move.wait()

    def mid_kernel(vis_ref, noise_ref, before_ref, after_ref, column_ref, left_ref, right_ref):
        firsts, lasts = [], []
        for n in range(n_img):
            for at, payload in ((0, before_ref), (far + tile_rows, after_ref)):
                pixels = payload[n, :, own:].astype(f32)
                column_ref[n, at : at + reach, :] = pixels[:, :tile_cols]
                column_ref[n, at + reach : at + far, :] = pixels[: far - reach, tile_cols:]
            column_ref[n, far : far + tile_rows, :] = vis_ref[n].astype(f32)
            for ref, lane in ((left_ref, 0), (right_ref, own - part)):
                at = n * tall
                ref[at : at + reach, :] = before_ref[n, :, lane : lane + part]
                ref[at + reach : at + reach + tile_rows, :] = noise_ref[n, :, lane : lane + part]
                ref[at + reach + tile_rows : at + tall, :] = after_ref[n, :, lane : lane + part]
            for at in range(0, taller, reach):
                block = column_ref[n, at : at + reach, :]
                firsts.append(block[:, :far])
                lasts.append(block[:, tile_cols - far :])
        for ref, blocks in ((left_ref, firsts), (right_ref, lasts)):
            gap = jnp.zeros((reach, part - len(blocks) * far), f32)
            ref[every:, :] = jnp.concatenate(blocks + [gap], axis=1).astype(bf16)

    def band_kernel(pair_ref, w_ref, wide_ref):
        wide_ref[...] = jnp.zeros_like(wide_ref)
        for r in range(side):
            block = pair_ref[r]
            for v in range(chunks):
                wide_ref[pl.ds(r * wide + 2 * v, side + 1), pl.ds(v * LANES, LANES)] = block
        w_ref[...] = wide_ref[...].astype(bf16)

    def inverse(u):
        u = u.astype(f32)
        return jnp.where(u > 0.0, 1.0 / jnp.log(u), 0.0)

    def placed(tmp_ref, out_ref, n, lane):
        for odd in range(2):
            mine, above, below = slots(odd, n)
            for v in range(tmp_ref.shape[0]):
                lanes = slice(lane + v * LANES, lane + (v + 1) * LANES)
                line = skipping(tmp_ref, v, odd, tall // 2)
                out_ref[above : above + some, lanes] = line[:some]
                out_ref[mine : mine + few, lanes] = line[some : some + few]
                out_ref[below : below + some, lanes] = line[some + few :]

    def draw_kernel(noise_ref, before_ref, after_ref, t_ref, tmp_ref):
        for n in range(n_img):
            for v in range(chunks):
                at = slice(v * LANES, (v + 1) * LANES)
                tmp_ref[v, :reach, :] = inverse(before_ref[n, :, at])
                tmp_ref[v, reach : reach + tile_rows, :] = inverse(noise_ref[n, :, at])
                tmp_ref[v, reach + tile_rows :, :] = inverse(after_ref[n, :, at])
            placed(tmp_ref, t_ref, n, 0)

    def odds(even, odd):
        even, odd = even * SMALL, odd * SMALL
        total = even + odd
        total = total + pltpu.roll(total, channels, 1)
        share = 1.0 / (SMALL + total)
        return even * share, odd * share

    def main_kernel(
        flag_ref, column_ref, before_ref, after_ref, w_ref, t_ref, bias_ref, vis_ref,
        recon_ref, pack_ref,
        img_ref, col_ref, samp_ref, edge_ref, tmp_ref, back_ref, a2_ref, p2_ref, g_ref, cmb_ref, sum_ref,
    ):
        half = every // 2
        mine = n_img * few
        for n in range(n_img):
            strips = []
            for ref in (before_ref, after_ref):
                at = n * (taller // reach) * far
                strips.append(
                    jnp.concatenate(
                        [
                            ref[every:, at + k * far : at + (k + 1) * far].astype(f32)
                            for k in range(taller // reach)
                        ],
                        axis=0,
                    )
                )
            img_ref[n, :, :broad] = jnp.concatenate([strips[0], column_ref[n], strips[1]], axis=1)
        for at, ref in ((0, before_ref), (1, after_ref)):
            for n in range(n_img):
                for v in range(edge):
                    tmp_ref[v] = inverse(ref[n * tall : (n + 1) * tall, v * LANES : (v + 1) * LANES])
                placed(tmp_ref, edge_ref, n, at * part)
        hidden = jnp.zeros((1, LANES), f32)
        for block in range(2):
            for odd in range(2):
                for n in range(n_img):
                    own_at, above, below = slots(odd, n)
                    line = windows(img_ref, n, odd, tall // 2, block * tile_cols)
                    col_ref[above : above + some, :] = line[:some]
                    col_ref[own_at : own_at + few, :] = line[some : some + few]
                    col_ref[below : below + some, :] = line[some + few :]
            a = col_ref[...].astype(bf16)
            for v in range(chunks):
                at = slice(v * LANES, (v + 1) * LANES)
                if v % 2 == 0:
                    pair = jnp.dot(a, w_ref[:, v * LANES : (v + 2) * LANES], preferred_element_type=f32)
                act = pair[:, v % 2 * LANES : (v % 2 + 1) * LANES] + bias_ref[...]
                lift = jnp.exp(act)
                first, second = lift[:half], lift[half:]
                inner = v >= edge if block == 0 else v < edge
                if inner:
                    to = (v - edge if block == 0 else v + edge) * LANES
                    probs = odds(first[:mine], second[:mine])
                    for odd in range(2):
                        p2_ref[odd * mine : (odd + 1) * mine, to : to + LANES] = probs[odd].astype(bf16)
                        hidden = hidden + jnp.sum(probs[odd], axis=0, keepdims=True)
                    t = t_ref[:, to : to + LANES]
                else:
                    to = (v if block == 0 else v) * LANES
                    t = edge_ref[:, to : to + LANES]
                cold = jnp.where(t == 0.0, 0.0, lift * t)
                cold = cold * cold
                samples = odds(cold[:half], cold[half:])
                for odd in range(2):
                    at_row = block * every + odd * half
                    samp_ref[at_row : at_row + half, at] = samples[odd].astype(bf16)
        for odd in range(2):
            for n in range(n_img):
                at = (odd * n_img + n) * few
                a2_ref[at : at + few, :] = windows(img_ref, n, reach + odd, few, reach).astype(bf16)

        down = lax.dot_general(
            samp_ref[...], w_ref[...], (((1,), (1,)), ((), ())), preferred_element_type=f32
        )
        down = jnp.concatenate([down, jnp.zeros((2 * every, -taps % LANES), f32)], axis=1)
        for block in range(2):
            for odd in range(2):
                for n in range(n_img):
                    own_at, above, below = (block * every + at for at in slots(odd, n))
                    to = (block * n_img + n) * tall
                    line = jnp.concatenate(
                        [down[above : above + some], down[own_at : own_at + few], down[below : below + some]], axis=0
                    )
                    for v in range(back_ref.shape[0]):
                        put_skipping(back_ref, v, to + odd, line[:, v * LANES : (v + 1) * LANES])
        p = lax.broadcasted_iota(jnp.int32, (high, wide), 0)
        q = lax.broadcasted_iota(jnp.int32, (high, wide), 1)
        inside = (
            ((p >= margin) | (flag_ref[2:3, :wide] == 0.0))
            & ((p < margin + tile_rows) | (flag_ref[3:4, :wide] == 0.0))
            & ((q >= margin) | (flag_ref[0:1, :wide] == 0.0))
            & ((q < margin + tile_cols) | (flag_ref[1:2, :wide] == 0.0))
        )
        seen = jnp.zeros((tile_rows, tile_cols), f32)
        gap = jnp.zeros((high, reach), f32)
        for n in range(n_img):
            totals = []
            for block in range(2):
                total = jnp.zeros((high, wide), f32)
                for r in range(side):
                    at = (block * n_img + n) * tall + reach - r
                    lane, over = r * wide, max((r + 1) * wide - LANES, 0)
                    if lane < LANES < lane + wide:
                        piece = jnp.concatenate(
                            [back_ref[0, at : at + high, lane:], back_ref[1, at : at + high, :over]], axis=1
                        )
                    else:
                        lane %= LANES
                        piece = back_ref[int(over > 0), at : at + high, lane : lane + wide]
                    total = total + piece
                totals.append(total)
            total = jnp.concatenate([totals[0][:, reach:], gap], axis=1) + jnp.concatenate(
                [gap, totals[1][:, : wide - reach]], axis=1
            )
            recon = (total + flag_ref[4:5, :wide]).astype(bf16).astype(f32)
            img_ref[n, :high, :wide] = jnp.where(inside, recon, 0.0)
            middle = img_ref[n, margin : margin + tile_rows, margin : margin + tile_cols]
            recon_ref[n] = middle.astype(bf16)
            seen = seen + (vis_ref[n].astype(f32) - middle)
        seen = jnp.sum(seen, keepdims=True)

        for odd in range(2):
            for n in range(n_img):
                at = (odd * n_img + n) * few
                col_ref[at : at + few, :] = windows(img_ref, n, odd, few, 0)
        a = col_ref[:rows, :].astype(bf16)
        a2_ref[rows:, :] = -a
        for v in range(chunks):
            at = slice(v * LANES, (v + 1) * LANES)
            if v % 2 == 0:
                pair = jnp.dot(a, w_ref[:, v * LANES : (v + 2) * LANES], preferred_element_type=f32)
            act = pair[:, v % 2 * LANES : (v % 2 + 1) * LANES] + bias_ref[...]
            lift = jnp.exp(act)
            probs = odds(lift[:mine], lift[mine:])
            for odd in range(2):
                to = rows + odd * mine
                p2_ref[to : to + mine, at] = probs[odd].astype(bf16)
                hidden = hidden - jnp.sum(probs[odd], axis=0, keepdims=True)
        g_ref[...] = lax.dot_general(
            a2_ref[...], p2_ref[...], (((0,), (0,)), ((), ())), preferred_element_type=f32
        )
        lane = lax.broadcasted_iota(jnp.int32, (side, LANES), 1)
        cmb_ref[...] = jnp.zeros_like(cmb_ref)
        for r in range(side):
            acc = g_ref[pl.ds(r * wide, side + 1), pl.ds(0, LANES)]
            for v in range(1, chunks):
                acc = acc + g_ref[pl.ds(r * wide + 2 * v, side + 1), pl.ds(v * LANES, LANES)]
            turned = pltpu.roll(acc, channels, 1)
            cmb_ref[r * side : (r + 1) * side, :] = jnp.where(
                lane < channels, acc[:side] + turned[1 : side + 1], turned[:side] + acc[1 : side + 1]
            )
        hidden = hidden + pltpu.roll(hidden, channels, 1)
        lane = lax.broadcasted_iota(jnp.int32, (quarter, LANES), 1)
        sum_ref[...] = jnp.zeros_like(sum_ref)
        for half, last in ((0, hidden), (1, jnp.broadcast_to(seen, (1, LANES)))):
            at, to = 2 * half * quarter, half * half_rows
            sum_ref[to : to + quarter, :] = jnp.where(
                lane < channels, cmb_ref[at : at + quarter, :], cmb_ref[at + quarter : at + 2 * quarter, :]
            )
            sum_ref[to + quarter : to + quarter + 1, :] = last
        sent(sum_ref, pack_ref)

    def sent(sum_ref, pack_ref):
        for half in range(2):
            at = half * half_rows + quarter
            last = sum_ref[at : at + 1, :]
            sum_ref[at + 1 : at + 2, :] = last - last.astype(bf16).astype(f32)
        packed = sum_ref[...].astype(bf16)
        for to in range(pack_ref.shape[0]):
            pack_ref[to] = packed

    def added(parts_ref, sum_ref):
        sum_ref[...] = jnp.sum(parts_ref[...].astype(f32), axis=0)
        for half in range(2):
            at = half * half_rows + quarter
            sum_ref[at : at + 1, :] += sum_ref[at + 1 : at + 2, :]

    def spread_kernel(parts_ref, pack_ref, sum_ref):
        added(parts_ref, sum_ref)
        sent(sum_ref, pack_ref)

    def finish_kernel(parts_ref, recon_in_ref, recon_ref, grad_ref, hid_ref, seen_ref, sum_ref, flat_ref):
        recon_ref[...] = recon_in_ref[...]
        added(parts_ref, sum_ref)
        sum_ref[...] = sum_ref[...] * scale
        for part in range(4):
            at, lane = part // 2 * half_rows, part % 2 * channels
            flat_ref[part * quarter : (part + 1) * quarter, :] = sum_ref[at : at + quarter, lane : lane + channels]
        for r in range(side):
            grad_ref[r] = flat_ref[r * side : (r + 1) * side, :]
        hid_ref[...] = sum_ref[quarter : quarter + 1, :channels]
        seen_ref[...] = sum_ref[half_rows + quarter : half_rows + quarter + 1, :1]

    taps_first = filters.astype(f32).transpose(1, 2, 0)
    pairs = jnp.concatenate(
        [jnp.pad(taps_first, ((0, 0), (0, 1), (0, 0))), jnp.pad(taps_first, ((0, 0), (1, 0), (0, 0)))],
        axis=2,
    )
    bias = jnp.concatenate([hidden_bias, hidden_bias])[None]
    col_at, row_at = lax.axis_index(COL), lax.axis_index(ROW)
    first, last = col_at == 0, col_at == lax.axis_size(COL) - 1
    top, bottom = row_at == 0, row_at == lax.axis_size(ROW) - 1
    line = lax.broadcasted_iota(jnp.int32, (8, LANES), 0)
    flags = jnp.zeros((8, LANES), f32)
    for at, value in enumerate((first, last, top, bottom, visible_unit_bias)):
        flags = jnp.where(line == at, jnp.asarray(value, f32), flags)

    payload = shape((n_img, reach, own + 2 * tile_cols), bf16)
    downward, upward = call(
        pack_kernel,
        (payload, payload),
        [pltpu.VMEM(images.shape, bf16), pltpu.SemaphoreType.DMA((3,))],
        "pack",
        left=(0, 1),
    )(in_hbm(images), in_hbm(unit_noise))
    before, after = edges(ROW, downward, upward)
    (w,) = call(
        band_kernel, (shape((taps, own), bf16),), [pltpu.VMEM((taps, own), f32)], "band"
    )(pairs)
    sideways = shape((every + reach, part), bf16)
    column, leftward, rightward = call(
        mid_kernel, (shape((n_img, taller, tile_cols), f32), sideways, sideways), [], "mid"
    )(images, unit_noise, before, after)

    left, right = edges(COL, rightward, leftward)
    (t,) = call(
        draw_kernel, (shape((every, own), f32),), [pltpu.VMEM((chunks, tall, LANES), f32)], "draw"
    )(unit_noise, before, after)
    sizes = [lax.axis_size(axes) for axes in GROUPS]
    recon, pack = call(
        main_kernel,
        (shape(images.shape, bf16), shape((sizes[0], part_rows, LANES), bf16)),
        [
            pltpu.VMEM((n_img, taller, LANES), f32),
            pltpu.VMEM((every, taps), f32),
            pltpu.VMEM((2 * every, own), bf16),
            pltpu.VMEM((every, 2 * part), f32),
            pltpu.VMEM((edge, tall, LANES), f32),
            pltpu.VMEM((-(-taps // LANES), 2 * every, LANES), f32),
            pltpu.VMEM((2 * rows, taps), bf16),
            pltpu.VMEM((2 * rows, own), bf16),
            pltpu.VMEM((taps, own), f32),
            pltpu.VMEM((4 * quarter, LANES), f32),
            pltpu.VMEM((part_rows, LANES), f32),
        ],
        "main",
    )(flags, column, left, right, w, t, bias, images)

    scratch = [pltpu.VMEM((part_rows, LANES), f32)]
    for axes, following in zip(GROUPS, sizes[1:] + [None]):
        parts = lax.all_to_all(pack, axes, 0, 0, tiled=True)
        if following:
            (pack,) = call(
                spread_kernel, (shape((following, part_rows, LANES), bf16),), scratch, "spread"
            )(parts)
    recon, grad, hidden, seen = call(
        finish_kernel,
        (
            shape(images.shape, bf16),
            shape((side, side, channels), f32),
            shape((1, channels), f32),
            shape((1, 1), f32),
        ),
        scratch + [pltpu.VMEM((4 * quarter, channels), f32)],
        "finish",
    )(parts, recon)
    return (recon, grad.transpose(2, 0, 1), hidden[0], seen[0, 0])


def solution(mesh):
    split = Mesh(
        mesh.devices.reshape(mesh.shape["img"], 2, 4, 2, 2, 2, 2, 2),
        ("img",) + ROW + COL,
    )
    placed = (P("img", ROW, COL), P(), P(), P(), P("img", ROW, COL))
    return jax.shard_map(
        body,
        mesh=split,
        in_specs=placed,
        out_specs=(P("img", ROW, COL), P(), P(), P()),
        check_vma=False,
    )
```
